32 devices in a mesh: dp: 2 (over x), tp: 16 (over y, z, core).
Axes of the slice: x: 2, y: 2, z: 4, core: 2. Of those that a mesh axis runs over, the one named last changes fastest.
Arguments:
- x: bfloat16 [4096, 2048], P('dp'), parts along dimension 0
- dy: bfloat16 [4096, 2048], P('dp'), parts along dimension 0
- gate: bfloat16 [4096, 8192], P('dp', 'tp'), parts along dimension 0
- up: bfloat16 [4096, 8192], P('dp', 'tp'), parts along dimension 0
- w_gate: bfloat16 [2048, 8192], P(None, 'tp')
- w_up: bfloat16 [2048, 8192], P(None, 'tp')
- w_down: bfloat16 [8192, 2048], P('tp')
Outputs:
- output 1: bfloat16 [4096, 2048], P('dp'), parts along dimension 0
- output 2: bfloat16 [4096, 8192], P('dp', 'tp'), parts along dimension 0
- output 3: bfloat16 [4096, 8192], P('dp', 'tp'), parts along dimension 0
- output 4: bfloat16 [16384, 2048], P(('dp', 'tp')), parts along dimension 0
There are 2 independent parts. The reference program is written for one: setup_inputs(seed, part) draws one part's arguments, and reference() takes and returns one part's arrays. A program takes and returns all parts, laid end to end along the dimension named above; an argument that names none is the same for every part.
All inputs are finite; a program needn't handle non-finite values.
Results may differ from the reference program's by a relative error of at most 0.012.
Values are sent between devices in bfloat16 or wider.
A program may use at most 2 GiB of HBM per device.

```python
import jax
import jax.numpy as jnp

ROWS = 2048
D = 2048
FF = 8192


def act(gate, up):
    return jax.nn.silu(gate) * up


def setup_inputs(seed: int = 0, part: int = 0) -> dict:
    kx, ky, ka, kb, kg, ku, kd = jax.random.split(jax.random.key(seed), 7)
    kx, ky, ka, kb = (jax.random.fold_in(k, part) for k in (kx, ky, ka, kb))
    drawn = {
        "x": jax.random.normal(kx, (ROWS, D), jnp.float32),
        "dy": jax.random.normal(ky, (ROWS, D), jnp.float32),
        "gate": jax.random.normal(ka, (ROWS, FF), jnp.float32),
        "up": jax.random.normal(kb, (ROWS, FF), jnp.float32),
        "w_gate": jax.random.normal(kg, (D, FF), jnp.float32) * D**-0.5,
        "w_up": jax.random.normal(ku, (D, FF), jnp.float32) * D**-0.5,
        "w_down": jax.random.normal(kd, (FF, D), jnp.float32) * FF**-0.5,
    }
    return {k: v.astype(jnp.bfloat16) for k, v in drawn.items()}


def reference(x, dy, gate, up, w_gate, w_up, w_down):
    hidden, back = jax.vjp(act, gate.astype(jnp.float32), up.astype(jnp.float32))
    d_hidden = jnp.dot(dy, w_down.T, preferred_element_type=jnp.float32)
    d_gate, d_up = (g.astype(jnp.bfloat16) for g in back(d_hidden))
    dx = jnp.dot(d_gate, w_gate.T, preferred_element_type=jnp.float32) + jnp.dot(d_up, w_up.T, preferred_element_type=jnp.float32)
    dw_gate = jnp.dot(x.T, d_gate, preferred_element_type=jnp.float32)
    dw_up = jnp.dot(x.T, d_up, preferred_element_type=jnp.float32)
    dw_down = jnp.dot(hidden.astype(jnp.bfloat16).T, dy, preferred_element_type=jnp.float32)
    return tuple(g.astype(jnp.bfloat16) for g in (dx, dw_gate, dw_up, dw_down))
```

```python
import functools

import jax
import jax.numpy as jnp
from jax import lax
from jax.experimental import pallas as pl
from jax.experimental.pallas import tpu as pltpu
from jax.sharding import PartitionSpec as P

MESH = pl.DeviceIdType.MESH
F32, BF16 = jnp.float32, jnp.bfloat16

M, D, F = 2048, 2048, 512
HALF = D // 2
W = D // 8
R = 64
S = M // R
TB = 256
NB = M // TB
LAG = 2
NS = 4

A1, A2, A3, B1, B2, B3, FAO, FAY, FBO, FBI, FB2, FD = range(12)
KINDS = 12
NT = (((1,), (1,)), ((), ()))
NN = (((1,), (0,)), ((), ()))


def dot(a, b, dims):
    return lax.dot_general(a, b, dims, preferred_element_type=F32)


def kernel(x_hbm, dy_hbm, gate_hbm, up_hbm, wg_hbm, wu_hbm, wd_hbm, dx_hbm, dwg_hbm, dwu_hbm, dwd_hbm,
           own, fin, term_r, ra1, ra2, ra3, rb1, rb2, rb3, term_s, sa1, sa2, sa3, sb1, sb2, sb3,
           wgu, wd, dyb, gb, ub, dgu, hid_t, tile, tile_t, dwb, dwdb,
           send, recv, tsend, trecv, wsem, bsem, tilesem, osem, dsem):
    me = lax.axis_index("tp")
    c, z, y = lax.rem(me, 2), lax.rem(me // 2, 4), me // 8
    at = lambda yy, zz, cc: (yy * 4 + zz) * 2 + cc
    mate = at(y, z, 1 - c)
    across = at(1 - y, z, c)
    inner = jnp.logical_or(z == 1, z == 2)
    outer = jnp.logical_not(inner)
    right_half = z // 2
    near = at(y, jnp.where(z == 0, 1, jnp.where(z == 1, 0, jnp.where(z == 2, 3, 2))), c)
    far = at(y, jnp.where(z == 1, 2, 1), c)
    root = right_half

    barrier = pltpu.get_barrier_semaphore()
    for peer in (mate, across, near):
        pl.semaphore_signal(barrier, inc=1, device_id={"tp": peer}, device_id_type=MESH)

    @pl.when(inner)
    def _():
        pl.semaphore_signal(barrier, inc=1, device_id={"tp": far}, device_id_type=MESH)

    wcopies = [
        pltpu.make_async_copy(wd_hbm, wd, wsem.at[0]),
        pltpu.make_async_copy(wg_hbm, wgu.at[:, pl.ds(0, F)], wsem.at[1]),
        pltpu.make_async_copy(wu_hbm, wgu.at[:, pl.ds(F, F)], wsem.at[2]),
    ]

    def block_copies(b):
        slot, rows = lax.rem(b, 2), pl.ds(b * TB, TB)
        return [
            pltpu.make_async_copy(dy_hbm.at[rows, :], dyb.at[slot], bsem.at[slot, 0]),
            pltpu.make_async_copy(gate_hbm.at[rows, :], gb.at[slot], bsem.at[slot, 1]),
            pltpu.make_async_copy(up_hbm.at[rows, :], ub.at[slot], bsem.at[slot, 2]),
        ]

    def tile_copy(ref, i):
        slot = lax.rem(i, 2)
        return pltpu.make_async_copy(ref.at[:, pl.ds(i * TB, TB)], tile.at[slot], tilesem.at[slot])

    wcopies[0].start()
    for copy in block_copies(0):
        copy.start()
    wcopies[1].start()
    wcopies[2].start()
    for copy in block_copies(1):
        copy.start()
    tile_copy(x_hbm, 0).start()
    tile_copy(x_hbm, 1).start()

    @pl.when(inner)
    def _():
        pl.semaphore_wait(barrier, 4)

    @pl.when(outer)
    def _():
        pl.semaphore_wait(barrier, 3)

    def term_copy(b):
        slot, rows = lax.rem(b, 2), pl.ds(b * TB, TB)
        return pltpu.make_async_remote_copy(
            term_s.at[slot], term_r.at[rows, :], tsend.at[slot], trecv.at[b],
            device_id={"tp": mate}, device_id_type=MESH)

    def terms(b):
        slot = lax.rem(b, 2)
        row = pl.multiple_of(b * TB, TB)
        rows = pl.ds(row, TB)

        @pl.when(b == 0)
        def _():
            wcopies[0].wait()

        for copy in block_copies(b):
            copy.wait()
        for n in range(F // 256):
            cols = slice(n * 256, (n + 1) * 256)
            dh = dot(dyb[slot], wd[cols, :], NT)
            g, u = gb[slot, :, cols].astype(F32), ub[slot, :, cols].astype(F32)
            sig = 1.0 / (1.0 + jnp.exp(-g))
            silu = g * sig
            du = dh * u
            dgu[rows, cols] = (du * sig + du * g * (sig * (1.0 - sig))).astype(BF16)
            dgu[rows, F + n * 256:F + (n + 1) * 256] = (dh * silu).astype(BF16)
            hid_t[cols, rows] = (silu * u).T.astype(BF16)

        @pl.when(b + 2 < NB)
        def _():
            for copy in block_copies(b + 2):
                copy.start()

        @pl.when(b == 0)
        def _():
            wcopies[1].wait()
            wcopies[2].wait()

        @pl.when(b >= 2)
        def _():
            term_copy(b - 2).wait_send()

        for n in range(HALF // 256):
            t = dot(dgu[rows, :], wgu[pl.ds(pl.multiple_of((1 - c) * HALF + n * 256, 256), 256), :], NT)
            term_s[slot, :, n * 256:(n + 1) * 256] = t.astype(BF16)
        term_copy(b).start()
        for n in range(HALF // 256):
            t = dot(dgu[rows, :], wgu[pl.ds(pl.multiple_of(c * HALF + n * 256, 256), 256), :], NT)
            own[rows, n * 256:(n + 1) * 256] = t

    def dw_copies(i):
        slot, rows = lax.rem(i, 2), pl.ds(i * TB, TB)
        return [
            pltpu.make_async_copy(dwb.at[slot, :, pl.ds(0, F)], dwg_hbm.at[rows, :], dsem.at[slot, 0]),
            pltpu.make_async_copy(dwb.at[slot, :, pl.ds(F, F)], dwu_hbm.at[rows, :], dsem.at[slot, 1]),
        ]

    def dw_gate_up(i):
        slot = lax.rem(i, 2)
        tile_copy(x_hbm, i).wait()
        for j in range(M // 256):
            tile_t[:, j * 256:(j + 1) * 256] = tile[slot, j * 256:(j + 1) * 256, :].T

        @pl.when(i + 2 < NB)
        def _():
            tile_copy(x_hbm, i + 2).start()

        @pl.when(i + 2 >= NB)
        def _():
            tile_copy(dy_hbm, i + 2 - NB).start()

        @pl.when(i >= 2)
        def _():
            for copy in dw_copies(i - 2):
                copy.wait()

        for n in range(2 * F // 256):
            dwb[slot, :, n * 256:(n + 1) * 256] = dot(tile_t[...], dgu[:, n * 256:(n + 1) * 256], NN).astype(BF16)
        for copy in dw_copies(i):
            copy.start()

    def dwd_copy(i):
        slot = lax.rem(i, 2)
        return pltpu.make_async_copy(dwdb.at[slot], dwd_hbm.at[:, pl.ds(i * TB, TB)], dsem.at[slot, 2])

    def dw_down(i):
        slot = lax.rem(i, 2)
        tile_copy(dy_hbm, i).wait()

        @pl.when(i >= 2)
        def _():
            dwd_copy(i - 2).wait()

        for n in range(F // 256):
            dwdb[slot, n * 256:(n + 1) * 256, :] = dot(hid_t[n * 256:(n + 1) * 256, :], tile[slot], NN).astype(BF16)

        @pl.when(i + 2 < NB)
        def _():
            tile_copy(dy_hbm, i + 2).start()

        dwd_copy(i).start()

    def part(ref, k, col=0, width=W):
        return ref.at[pl.ds(pl.multiple_of(k * R, R), R), pl.ds(col, width)]

    base = pl.multiple_of(c * HALF, HALF)
    col_a = pl.multiple_of(y * W, W)
    col_a_other = pl.multiple_of((1 - y) * W, W)
    col_b = pl.multiple_of(2 * W + root * W, W)
    col_b_other = pl.multiple_of(2 * W + (1 - root) * W, W)

    def message(kind, k, there=False):
        slot = lax.rem(k, NS)
        fin_own = lambda col, width=W: part(fin, k, pl.multiple_of(base + col, W), width)
        a_col = col_a_other if there else col_a
        src, dst, peer = {
            A1: (sa1.at[slot], part(ra1, k), across),
            A2: (sa2.at[slot], part(ra2, k), near),
            A3: (sa3.at[slot], part(ra3, k), far),
            B1: (sb1.at[slot], part(rb1, k, 0, 2 * W), near),
            B2: (sb2.at[slot], part(rb2, k), far),
            B3: (sb3.at[slot], part(rb3, k), across),
            FAO: (fin_own(col_a), fin_own(col_a), near),
            FAY: (fin_own(a_col), fin_own(a_col), across),
            FBO: (fin_own(col_b), fin_own(col_b), near),
            FBI: (fin_own(col_b_other if there else col_b), fin_own(col_b_other if there else col_b), far),
            FB2: (fin_own(col_b_other), fin_own(col_b_other), near),
            FD: None,
        }[kind] or (None, None, None)
        if kind == FD:
            col = pl.multiple_of((1 - c) * HALF if there else c * HALF, HALF)
            src = dst = part(fin, k, col, HALF)
            peer = mate
        return pltpu.make_async_remote_copy(
            src, dst, send.at[kind, slot], recv.at[kind, k], device_id={"tp": peer}, device_id_type=MESH)

    def free(kind, k):
        @pl.when(k >= NS)
        def _():
            message(kind, k - NS).wait_send()

    def arrived(kind, k):
        message(kind, k, there=True).wait_recv()

    def ld(ref, k, col=0, width=W):
        return ref[pl.ds(pl.multiple_of(k * R, R), R), pl.ds(col, width)].astype(F32)

    def st(ref, k, col, value, width=W):
        ref[pl.ds(pl.multiple_of(k * R, R), R), pl.ds(col, width)] = value

    def e1(k):
        @pl.when(lax.rem(k, TB // R) == 0)
        def _():
            term_copy(k // (TB // R)).wait_recv()

        slot = lax.rem(k, NS)
        free(A1, k)
        sa1[slot] = (ld(own, k, col_a_other) + ld(term_r, k, col_a_other)).astype(BF16)
        message(A1, k).start()

        @pl.when(outer)
        def _():
            free(B1, k)
            sb1[slot] = (ld(own, k, 2 * W, 2 * W) + ld(term_r, k, 2 * W, 2 * W)).astype(BF16)
            message(B1, k).start()

        @pl.when(inner)
        def _():
            st(own, k, 2 * W, ld(own, k, 2 * W, 2 * W) + ld(term_r, k, 2 * W, 2 * W), 2 * W)

        st(own, k, col_a, ld(own, k, col_a) + ld(term_r, k, col_a))

    def e2(k):
        slot = lax.rem(k, NS)

        @pl.when(inner)
        def _():
            arrived(B1, k)
            free(B2, k)
            other = pl.multiple_of((1 - root) * W, W)
            sb2[slot] = (ld(own, k, col_b_other) + ld(rb1, k, other)).astype(BF16)
            message(B2, k).start()
            st(own, k, col_b, ld(own, k, col_b) + ld(rb1, k, pl.multiple_of(root * W, W)))

        arrived(A1, k)

        @pl.when(outer)
        def _():
            free(A2, k)
            sa2[slot] = (ld(own, k, col_a) + ld(ra1, k)).astype(BF16)
            message(A2, k).start()

        @pl.when(inner)
        def _():
            st(own, k, col_a, ld(own, k, col_a) + ld(ra1, k))

    def e3(k):
        slot = lax.rem(k, NS)

        @pl.when(inner)
        def _():
            arrived(B2, k)
            free(B3, k)
            sb3[slot] = (ld(own, k, col_b) + ld(rb2, k)).astype(BF16)
            message(B3, k).start()
            arrived(A2, k)
            free(A3, k)
            sa3[slot] = (ld(own, k, col_a) + ld(ra2, k)).astype(BF16)
            message(A3, k).start()

    def e4(k):
        slot = lax.rem(k, NS)

        @pl.when(inner)
        def _():
            arrived(B3, k)
            st(fin, k, pl.multiple_of(base + col_b, W), (sb3[slot].astype(F32) + ld(rb3, k)).astype(BF16))
            free(FBI, k)
            message(FBI, k).start()
            free(FBO, k)
            message(FBO, k).start()
            arrived(A3, k)
            st(fin, k, pl.multiple_of(base + col_a, W), (sa3[slot].astype(F32) + ld(ra3, k)).astype(BF16))
            free(FAO, k)
            message(FAO, k).start()
            free(FAY, k)
            message(FAY, k).start()

    def e5(k):
        @pl.when(inner)
        def _():
            arrived(FBI, k)
            free(FB2, k)
            message(FB2, k).start()

        @pl.when(outer)
        def _():
            arrived(FAO, k)
            free(FAY, k)
            message(FAY, k).start()

    def e6(k):
        @pl.when(outer)
        def _():
            arrived(FBO, k)
            arrived(FB2, k)

        arrived(FAY, k)
        free(FD, k)
        message(FD, k).start()

    def out_copy(k):
        rows = pl.ds(pl.multiple_of(k * R, R), R)
        return pltpu.make_async_copy(fin.at[rows, :], dx_hbm.at[rows, :], osem.at[lax.rem(k, NS)])

    def e7(k):
        arrived(FD, k)

        @pl.when(k >= NS)
        def _():
            out_copy(k - NS).wait()

        out_copy(k).start()

    events = [(e1, 1), (e2, 1 + LAG), (e3, 1 + 2 * LAG), (e4, 1 + 3 * LAG), (e5, 1 + 4 * LAG), (e6, 1 + 5 * LAG), (e7, 2 + 5 * LAG)]
    steps = S + 2 + 5 * LAG

    def step(s, _):
        for event, offset in events:
            @pl.when(jnp.logical_and(s >= offset, s < S + offset))
            def _(event=event, offset=offset):
                event(s - offset)

        @pl.when(jnp.logical_and(lax.rem(s, 2) == 0, s < 2 * NB))
        def _():
            terms(s // 2)

        @pl.when(jnp.logical_and(s >= 2 * NB, s < 3 * NB))
        def _():
            dw_gate_up(s - 2 * NB)

        @pl.when(jnp.logical_and(s >= 3 * NB, s < 4 * NB))
        def _():
            dw_down(s - 3 * NB)

        return 0

    lax.fori_loop(0, steps, step, 0)

    for b in (NB - 2, NB - 1):
        term_copy(b).wait_send()
        for copy in dw_copies(b):
            copy.wait()
        dwd_copy(b).wait()

    def drain(kinds):
        for kind in kinds:
            for k in range(S - NS, S):
                message(kind, k).wait_send()

    drain((A1, FAY, FD))

    @pl.when(inner)
    def _():
        drain((A3, B2, B3, FAO, FBO, FBI, FB2))

    @pl.when(outer)
    def _():
        drain((A2, B1))

    for k in range(S - NS, S):
        out_copy(k).wait()


def solution(mesh):
    def step(x, dy, gate, up, w_gate, w_up, w_down):
        vmem = pltpu.VMEM
        dma = pltpu.SemaphoreType.DMA
        scratch = [
            vmem((M, HALF), F32), vmem((M, D), BF16), vmem((M, HALF), BF16),
            vmem((M, W), BF16), vmem((M, W), BF16), vmem((M, W), BF16),
            vmem((M, 2 * W), BF16), vmem((M, W), BF16), vmem((M, W), BF16),
            vmem((2, TB, HALF), BF16),
            vmem((NS, R, W), BF16), vmem((NS, R, W), BF16), vmem((NS, R, W), BF16),
            vmem((NS, R, 2 * W), BF16), vmem((NS, R, W), BF16), vmem((NS, R, W), BF16),
            vmem((D, 2 * F), BF16), vmem((F, D), BF16),
            vmem((2, TB, D), BF16), vmem((2, TB, F), BF16), vmem((2, TB, F), BF16),
            vmem((M, 2 * F), BF16), vmem((F, M), BF16),
            vmem((2, M, TB), BF16), vmem((TB, M), BF16), vmem((2, TB, 2 * F), BF16), vmem((2, F, TB), BF16),
            dma((KINDS, NS)), dma((KINDS, S)), dma((2,)), dma((NB,)), dma((3,)), dma((2, 3)), dma((2,)), dma((NS,)), dma((2, 3)),
        ]
        anywhere = pl.BlockSpec(memory_space=pl.ANY)
        shape = jax.ShapeDtypeStruct
        return pl.pallas_call(
            kernel,
            out_shape=(shape((M, D), BF16), shape((D, F), BF16), shape((D, F), BF16), shape((F, D), BF16)),
            in_specs=[anywhere] * 7,
            out_specs=(anywhere,) * 4,
            scratch_shapes=scratch,
            compiler_params=pltpu.CompilerParams(collective_id=0, has_side_effects=True, vmem_limit_bytes=64 * 1024 * 1024 - 65536),
        )(x, dy, gate, up, w_gate, w_up, w_down)

    tokens, columns, rows = P("dp", None), P(None, "tp"), P("tp", None)
    return jax.shard_map(
        step,
        mesh=mesh,
        in_specs=(tokens, tokens, P("dp", "tp"), P("dp", "tp"), columns, columns, rows),
        out_specs=(tokens, P("dp", "tp"), P("dp", "tp"), P(("dp", "tp"), None)),
        check_vma=False,
    )
```

```python
import functools

import jax
import jax.numpy as jnp
from jax import lax
from jax.experimental import pallas as pl
from jax.experimental.pallas import tpu as pltpu
from jax.sharding import PartitionSpec as P

MESH = pl.DeviceIdType.MESH
F32, BF16 = jnp.float32, jnp.bfloat16

M, D, F = 2048, 2048, 512
HALF = D // 2
W = D // 8
R = 64
S = M // R
TB = 256
NB = M // TB
LAG = 2
NS = 4
LIMIT = 48 * 1024 * 1024

A1, A2, A3, B1, B2, B3, FAO, FAY, FBO, FBI, FB2, FD = range(12)
KINDS = 12
NT = (((1,), (1,)), ((), ()))
NN = (((1,), (0,)), ((), ()))


def dot(a, b, dims):
    return lax.dot_general(a, b, dims, preferred_element_type=F32)


def kernel(x_hbm, dy_hbm, gate_hbm, up_hbm, wg_hbm, wu_hbm, wd_hbm, fin, dwg, dwu, dwd,
           own, term_r, ra1, ra2, ra3, rb1, rb2, rb3, term_s, sa1, sa2, sa3, sb1, sb2, sb3,
           wgu, wd, dyb, gb, ub, dgu, hid_t, tile, tile_t,
           send, recv, tsend, trecv, wsem, bsem, tilesem):
    me = lax.axis_index("tp")
    c, z, y = lax.rem(me, 2), lax.rem(me // 2, 4), me // 8
    at = lambda yy, zz, cc: (yy * 4 + zz) * 2 + cc
    mate = at(y, z, 1 - c)
    across = at(1 - y, z, c)
    inner = jnp.logical_or(z == 1, z == 2)
    outer = jnp.logical_not(inner)
    right_half = z // 2
    near = at(y, jnp.where(z == 0, 1, jnp.where(z == 1, 0, jnp.where(z == 2, 3, 2))), c)
    far = at(y, jnp.where(z == 1, 2, 1), c)
    root = right_half

    barrier = pltpu.get_barrier_semaphore()
    for peer in (mate, across, near):
        pl.semaphore_signal(barrier, inc=1, device_id={"tp": peer}, device_id_type=MESH)

    @pl.when(inner)
    def _():
        pl.semaphore_signal(barrier, inc=1, device_id={"tp": far}, device_id_type=MESH)

    wcopies = [
        pltpu.make_async_copy(wd_hbm, wd, wsem.at[0]),
        pltpu.make_async_copy(wg_hbm, wgu.at[:, pl.ds(0, F)], wsem.at[1]),
        pltpu.make_async_copy(wu_hbm, wgu.at[:, pl.ds(F, F)], wsem.at[2]),
    ]

    def block_copies(b):
        slot, rows = lax.rem(b, 2), pl.ds(b * TB, TB)
        return [
            pltpu.make_async_copy(dy_hbm.at[rows, :], dyb.at[slot], bsem.at[slot, 0]),
            pltpu.make_async_copy(gate_hbm.at[rows, :], gb.at[slot], bsem.at[slot, 1]),
            pltpu.make_async_copy(up_hbm.at[rows, :], ub.at[slot], bsem.at[slot, 2]),
        ]

    def tile_copy(ref, i):
        slot = lax.rem(i, 2)
        return pltpu.make_async_copy(ref.at[:, pl.ds(i * TB, TB)], tile.at[slot], tilesem.at[slot])

    wcopies[0].start()
    for copy in block_copies(0):
        copy.start()
    wcopies[1].start()
    wcopies[2].start()
    for copy in block_copies(1):
        copy.start()
    tile_copy(x_hbm, 0).start()
    tile_copy(x_hbm, 1).start()

    @pl.when(inner)
    def _():
        pl.semaphore_wait(barrier, 4)

    @pl.when(outer)
    def _():
        pl.semaphore_wait(barrier, 3)

    def term_copy(b):
        slot, rows = lax.rem(b, 2), pl.ds(b * TB, TB)
        return pltpu.make_async_remote_copy(
            term_s.at[slot], term_r.at[rows, :], tsend.at[slot], trecv.at[b],
            device_id={"tp": mate}, device_id_type=MESH)

    def terms(b):
        slot = lax.rem(b, 2)
        row = pl.multiple_of(b * TB, TB)
        rows = pl.ds(row, TB)

        @pl.when(b == 0)
        def _():
            wcopies[0].wait()

        for copy in block_copies(b):
            copy.wait()
        for n in range(F // 256):
            cols = slice(n * 256, (n + 1) * 256)
            dh = dot(dyb[slot], wd[cols, :], NT)
            g, u = gb[slot, :, cols].astype(F32), ub[slot, :, cols].astype(F32)
            sig = 1.0 / (1.0 + jnp.exp(-g))
            silu = g * sig
            du = dh * u
            dgu[rows, cols] = (du * sig + du * g * (sig * (1.0 - sig))).astype(BF16)
            dgu[rows, F + n * 256:F + (n + 1) * 256] = (dh * silu).astype(BF16)
            hid_t[cols, rows] = (silu * u).T.astype(BF16)

        @pl.when(b + 2 < NB)
        def _():
            for copy in block_copies(b + 2):
                copy.start()

        @pl.when(b == 0)
        def _():
            wcopies[1].wait()
            wcopies[2].wait()

        @pl.when(b >= 2)
        def _():
            term_copy(b - 2).wait_send()

        for n in range(HALF // 256):
            t = dot(dgu[rows, :], wgu[pl.ds(pl.multiple_of((1 - c) * HALF + n * 256, 256), 256), :], NT)
            term_s[slot, :, n * 256:(n + 1) * 256] = t.astype(BF16)
        term_copy(b).start()
        for n in range(HALF // 256):
            t = dot(dgu[rows, :], wgu[pl.ds(pl.multiple_of(c * HALF + n * 256, 256), 256), :], NT)
            own[rows, n * 256:(n + 1) * 256] = t

    def dw_gate_up(i):
        slot = lax.rem(i, 2)
        tile_copy(x_hbm, i).wait()
        for j in range(M // 256):
            tile_t[:, j * 256:(j + 1) * 256] = tile[slot, j * 256:(j + 1) * 256, :].T

        @pl.when(i + 2 < NB)
        def _():
            tile_copy(x_hbm, i + 2).start()

        @pl.when(i + 2 >= NB)
        def _():
            tile_copy(dy_hbm, i + 2 - NB).start()

        rows = pl.ds(pl.multiple_of(i * TB, TB), TB)
        for n in range(F // 256):
            cols = slice(n * 256, (n + 1) * 256)
            dwg[rows, cols] = dot(tile_t[...], dgu[:, n * 256:(n + 1) * 256], NN).astype(BF16)
            dwu[rows, cols] = dot(tile_t[...], dgu[:, F + n * 256:F + (n + 1) * 256], NN).astype(BF16)

    def dw_down(i):
        slot = lax.rem(i, 2)
        tile_copy(dy_hbm, i).wait()

        cols = pl.ds(pl.multiple_of(i * TB, TB), TB)
        for n in range(F // 256):
            dwd[n * 256:(n + 1) * 256, cols] = dot(hid_t[n * 256:(n + 1) * 256, :], tile[slot], NN).astype(BF16)

        @pl.when(i + 2 < NB)
        def _():
            tile_copy(dy_hbm, i + 2).start()

    def part(ref, k, col=0, width=W):
        return ref.at[pl.ds(pl.multiple_of(k * R, R), R), pl.ds(col, width)]

    base = pl.multiple_of(c * HALF, HALF)
    col_a = pl.multiple_of(y * W, W)
    col_a_other = pl.multiple_of((1 - y) * W, W)
    col_b = pl.multiple_of(2 * W + root * W, W)
    col_b_other = pl.multiple_of(2 * W + (1 - root) * W, W)

    def message(kind, k, there=False):
        slot = lax.rem(k, NS)
        fin_own = lambda col, width=W: part(fin, k, pl.multiple_of(base + col, W), width)
        a_col = col_a_other if there else col_a
        src, dst, peer = {
            A1: (sa1.at[slot], part(ra1, k), across),
            A2: (sa2.at[slot], part(ra2, k), near),
            A3: (sa3.at[slot], part(ra3, k), far),
            B1: (sb1.at[slot], part(rb1, k, 0, 2 * W), near),
            B2: (sb2.at[slot], part(rb2, k), far),
            B3: (sb3.at[slot], part(rb3, k), across),
            FAO: (fin_own(col_a), fin_own(col_a), near),
            FAY: (fin_own(a_col), fin_own(a_col), across),
            FBO: (fin_own(col_b), fin_own(col_b), near),
            FBI: (fin_own(col_b_other if there else col_b), fin_own(col_b_other if there else col_b), far),
            FB2: (fin_own(col_b_other), fin_own(col_b_other), near),
            FD: None,
        }[kind] or (None, None, None)
        if kind == FD:
            col = pl.multiple_of((1 - c) * HALF if there else c * HALF, HALF)
            src = dst = part(fin, k, col, HALF)
            peer = mate
        return pltpu.make_async_remote_copy(
            src, dst, send.at[kind, slot], recv.at[kind, k], device_id={"tp": peer}, device_id_type=MESH)

    def free(kind, k):
        @pl.when(k >= NS)
        def _():
            message(kind, k - NS).wait_send()

    def arrived(kind, k):
        message(kind, k, there=True).wait_recv()

    def ld(ref, k, col=0, width=W):
        return ref[pl.ds(pl.multiple_of(k * R, R), R), pl.ds(col, width)].astype(F32)

    def st(ref, k, col, value, width=W):
        ref[pl.ds(pl.multiple_of(k * R, R), R), pl.ds(col, width)] = value

    def e1(k):
        @pl.when(lax.rem(k, TB // R) == 0)
        def _():
            term_copy(k // (TB // R)).wait_recv()

        slot = lax.rem(k, NS)
        free(A1, k)
        sa1[slot] = (ld(own, k, col_a_other) + ld(term_r, k, col_a_other)).astype(BF16)
        message(A1, k).start()

        @pl.when(outer)
        def _():
            free(B1, k)
            sb1[slot] = (ld(own, k, 2 * W, 2 * W) + ld(term_r, k, 2 * W, 2 * W)).astype(BF16)
            message(B1, k).start()

        @pl.when(inner)
        def _():
            st(own, k, 2 * W, ld(own, k, 2 * W, 2 * W) + ld(term_r, k, 2 * W, 2 * W), 2 * W)

        st(own, k, col_a, ld(own, k, col_a) + ld(term_r, k, col_a))

    def e2(k):
        slot = lax.rem(k, NS)

        @pl.when(inner)
        def _():
            arrived(B1, k)
            free(B2, k)
            other = pl.multiple_of((1 - root) * W, W)
            sb2[slot] = (ld(own, k, col_b_other) + ld(rb1, k, other)).astype(BF16)
            message(B2, k).start()
            st(own, k, col_b, ld(own, k, col_b) + ld(rb1, k, pl.multiple_of(root * W, W)))

        arrived(A1, k)

        @pl.when(outer)
        def _():
            free(A2, k)
            sa2[slot] = (ld(own, k, col_a) + ld(ra1, k)).astype(BF16)
            message(A2, k).start()

        @pl.when(inner)
        def _():
            st(own, k, col_a, ld(own, k, col_a) + ld(ra1, k))

    def e3(k):
        slot = lax.rem(k, NS)

        @pl.when(inner)
        def _():
            arrived(B2, k)
            free(B3, k)
            sb3[slot] = (ld(own, k, col_b) + ld(rb2, k)).astype(BF16)
            message(B3, k).start()
            arrived(A2, k)
            free(A3, k)
            sa3[slot] = (ld(own, k, col_a) + ld(ra2, k)).astype(BF16)
            message(A3, k).start()

    def e4(k):
        slot = lax.rem(k, NS)

        @pl.when(inner)
        def _():
            arrived(B3, k)
            st(fin, k, pl.multiple_of(base + col_b, W), (sb3[slot].astype(F32) + ld(rb3, k)).astype(BF16))
            free(FBI, k)
            message(FBI, k).start()
            free(FBO, k)
            message(FBO, k).start()
            arrived(A3, k)
            st(fin, k, pl.multiple_of(base + col_a, W), (sa3[slot].astype(F32) + ld(ra3, k)).astype(BF16))
            free(FAO, k)
            message(FAO, k).start()
            free(FAY, k)
            message(FAY, k).start()

    def e5(k):
        @pl.when(inner)
        def _():
            arrived(FBI, k)
            free(FB2, k)
            message(FB2, k).start()

        @pl.when(outer)
        def _():
            arrived(FAO, k)
            free(FAY, k)
            message(FAY, k).start()

    def e6(k):
        @pl.when(outer)
        def _():
            arrived(FBO, k)
            arrived(FB2, k)

        arrived(FAY, k)
        free(FD, k)
        message(FD, k).start()

    def e7(k):
        arrived(FD, k)

    events = [(e1, 1), (e2, 1 + LAG), (e3, 1 + 2 * LAG), (e4, 1 + 3 * LAG), (e5, 1 + 4 * LAG), (e6, 1 + 5 * LAG), (e7, 2 + 5 * LAG)]
    steps = S + 2 + 5 * LAG

    def step(s, _):
        for event, offset in events:
            @pl.when(jnp.logical_and(s >= offset, s < S + offset))
            def _(event=event, offset=offset):
                event(s - offset)

        @pl.when(jnp.logical_and(lax.rem(s, 2) == 0, s < 2 * NB))
        def _():
            terms(s // 2)

        @pl.when(jnp.logical_and(s >= 2 * NB, s < 3 * NB))
        def _():
            dw_gate_up(s - 2 * NB)

        @pl.when(jnp.logical_and(s >= 3 * NB, s < 4 * NB))
        def _():
            dw_down(s - 3 * NB)

        return 0

    lax.fori_loop(0, steps, step, 0)

    for b in (NB - 2, NB - 1):
        term_copy(b).wait_send()

    def drain(kinds):
        for kind in kinds:
            for k in range(S - NS, S):
                message(kind, k).wait_send()

    drain((A1, FAY, FD))

    @pl.when(inner)
    def _():
        drain((A3, B2, B3, FAO, FBO, FBI, FB2))

    @pl.when(outer)
    def _():
        drain((A2, B1))


PIECES = 4


def write_out(*refs):
    sources, targets, sems = refs[:4], refs[4:8], refs[8]
    copies = []
    for i, (source, target) in enumerate(zip(sources, targets)):
        size = source.shape[0] // PIECES
        for j in range(PIECES):
            rows = pl.ds(j * size, size)
            copies.append(pltpu.make_async_copy(source.at[rows, :], target.at[rows, :], sems.at[i, j]))
    for copy in copies:
        copy.start()
    for copy in copies:
        copy.wait()


def solution(mesh):
    def step(x, dy, gate, up, w_gate, w_up, w_down):
        vmem = pltpu.VMEM
        dma = pltpu.SemaphoreType.DMA
        scratch = [
            vmem((M, HALF), F32), vmem((M, HALF), BF16),
            vmem((M, W), BF16), vmem((M, W), BF16), vmem((M, W), BF16),
            vmem((M, 2 * W), BF16), vmem((M, W), BF16), vmem((M, W), BF16),
            vmem((2, TB, HALF), BF16),
            vmem((NS, R, W), BF16), vmem((NS, R, W), BF16), vmem((NS, R, W), BF16),
            vmem((NS, R, 2 * W), BF16), vmem((NS, R, W), BF16), vmem((NS, R, W), BF16),
            vmem((D, 2 * F), BF16), vmem((F, D), BF16),
            vmem((2, TB, D), BF16), vmem((2, TB, F), BF16), vmem((2, TB, F), BF16),
            vmem((M, 2 * F), BF16), vmem((F, M), BF16),
            vmem((2, M, TB), BF16), vmem((TB, M), BF16),
            dma((KINDS, NS)), dma((KINDS, S)), dma((2,)), dma((NB,)), dma((3,)), dma((2, 3)), dma((2,)),
        ]
        anywhere = pl.BlockSpec(memory_space=pl.ANY)
        shape = jax.ShapeDtypeStruct
        shapes = ((M, D), (D, F), (D, F), (F, D))
        grads = pl.pallas_call(
            kernel,
            out_shape=tuple(vmem(dims, BF16) for dims in shapes),
            in_specs=[anywhere] * 7,
            out_specs=(pl.BlockSpec(memory_space=vmem),) * 4,
            scratch_shapes=scratch,
            compiler_params=pltpu.CompilerParams(collective_id=0, has_side_effects=True, vmem_limit_bytes=LIMIT),
        )(x, dy, gate, up, w_gate, w_up, w_down)
        return pl.pallas_call(
            write_out,
            out_shape=tuple(shape(dims, BF16) for dims in shapes),
            in_specs=[pl.BlockSpec(memory_space=vmem)] * 4,
            out_specs=(anywhere,) * 4,
            scratch_shapes=[dma((4, PIECES))],
            compiler_params=pltpu.CompilerParams(vmem_limit_bytes=1 << 20),
        )(*grads)

    tokens, columns, rows = P("dp", None), P(None, "tp"), P("tp", None)
    return jax.shard_map(
        step,
        mesh=mesh,
        in_specs=(tokens, tokens, P("dp", "tp"), P("dp", "tp"), columns, columns, rows),
        out_specs=(tokens, P("dp", "tp"), P("dp", "tp"), P(("dp", "tp"), None)),
        check_vma=False,
    )
```

```python
import functools

import jax
import jax.numpy as jnp
from jax import lax
from jax.experimental import pallas as pl
from jax.experimental.pallas import tpu as pltpu
from jax.sharding import PartitionSpec as P

MESH = pl.DeviceIdType.MESH
F32, BF16 = jnp.float32, jnp.bfloat16

M, D, F = 2048, 2048, 512
HALF = D // 2
WA, WB = 640, 384
R = 64
H = R // 2
S = M // R
TB = 256
NB = M // TB
A_AT = (1, 5, 7, 9, 13, 18)
B_AT = (3, 5, 7, 10, 12, 16)
C_AT = (1, 3, 5, 8, 10, 12, 14, 18)
NS = 4
LIMIT = 48 * 1024 * 1024

A1, A2, A3, FAO, FAY, B1, B2, B3, FBO, FBI, FB2, C1, C2, C3, C4, FC1, FC2, FC3, FDA, FDB = range(20)
ROW = {kind: row for row, kinds in enumerate((
    (A1,), (A2,), (A3,), (FAO,), (FAY,), (B1, C1), (B2, C2), (B3, C3), (FBO, C4), (FBI, FC2), (FB2, FC3), (FC1,), (FDA,), (FDB,)
)) for kind in kinds}
ROWS = 14
NT = (((1,), (1,)), ((), ()))
NN = (((1,), (0,)), ((), ()))


def dot(a, b, dims):
    return lax.dot_general(a, b, dims, preferred_element_type=F32)


def kernel(x_hbm, dy_hbm, gate_hbm, up_hbm, wg_hbm, wu_hbm, wd_hbm, fin, dwg, dwu, dwd,
           own, term_r, ra1, ra2, ra3, rb1, rb2, rb3, rb4, term_s, sa1, sa2, sa3, sb1, sb2, sb3, sb4,
           wgu, wd, dyb, gb, ub, dgu, hid_t, tile, tile_t,
           send, recv, tsend, trecv, wsem, bsem, tilesem):
    me = lax.axis_index("tp")
    c, z, y = lax.rem(me, 2), lax.rem(me // 2, 4), me // 8
    at = lambda yy, zz, cc: (yy * 4 + zz) * 2 + cc
    mate = at(y, z, 1 - c)
    across = at(1 - y, z, c)
    inner = jnp.logical_or(z == 1, z == 2)
    outer = jnp.logical_not(inner)
    right_half = z // 2
    near = at(y, jnp.where(z == 0, 1, jnp.where(z == 1, 0, jnp.where(z == 2, 3, 2))), c)
    far = at(y, jnp.where(z == 1, 2, 1), c)
    root = right_half

    barrier = pltpu.get_barrier_semaphore()
    for peer in (mate, across, near):
        pl.semaphore_signal(barrier, inc=1, device_id={"tp": peer}, device_id_type=MESH)

    @pl.when(inner)
    def _():
        pl.semaphore_signal(barrier, inc=1, device_id={"tp": far}, device_id_type=MESH)

    wcopies = [
        pltpu.make_async_copy(wd_hbm, wd, wsem.at[0]),
        pltpu.make_async_copy(wg_hbm, wgu.at[:, pl.ds(0, F)], wsem.at[1]),
        pltpu.make_async_copy(wu_hbm, wgu.at[:, pl.ds(F, F)], wsem.at[2]),
    ]

    def block_copies(b):
        slot, rows = lax.rem(b, 2), pl.ds(b * TB, TB)
        return [
            pltpu.make_async_copy(dy_hbm.at[rows, :], dyb.at[slot], bsem.at[slot, 0]),
            pltpu.make_async_copy(gate_hbm.at[rows, :], gb.at[slot], bsem.at[slot, 1]),
            pltpu.make_async_copy(up_hbm.at[rows, :], ub.at[slot], bsem.at[slot, 2]),
        ]

    def tile_copy(ref, i):
        slot = lax.rem(i, 2)
        return pltpu.make_async_copy(ref.at[:, pl.ds(i * TB, TB)], tile.at[slot], tilesem.at[slot])

    wcopies[0].start()
    for copy in block_copies(0):
        copy.start()
    wcopies[1].start()
    wcopies[2].start()
    for copy in block_copies(1):
        copy.start()
    tile_copy(x_hbm, 0).start()
    tile_copy(x_hbm, 1).start()

    @pl.when(inner)
    def _():
        pl.semaphore_wait(barrier, 4)

    @pl.when(outer)
    def _():
        pl.semaphore_wait(barrier, 3)

    def term_copy(b):
        slot, rows = lax.rem(b, 2), pl.ds(b * TB, TB)
        return pltpu.make_async_remote_copy(
            term_s.at[slot], term_r.at[rows, :], tsend.at[slot], trecv.at[b],
            device_id={"tp": mate}, device_id_type=MESH)

    def terms(b):
        slot = lax.rem(b, 2)
        row = pl.multiple_of(b * TB, TB)
        rows = pl.ds(row, TB)

        @pl.when(b == 0)
        def _():
            wcopies[0].wait()

        for copy in block_copies(b):
            copy.wait()
        for n in range(F // 256):
            cols = slice(n * 256, (n + 1) * 256)
            dh = dot(dyb[slot], wd[cols, :], NT)
            g, u = gb[slot, :, cols].astype(F32), ub[slot, :, cols].astype(F32)
            sig = 1.0 / (1.0 + jnp.exp(-g))
            silu = g * sig
            du = dh * u
            dgu[rows, cols] = (du * sig + du * g * (sig * (1.0 - sig))).astype(BF16)
            dgu[rows, F + n * 256:F + (n + 1) * 256] = (dh * silu).astype(BF16)
            hid_t[cols, rows] = (silu * u).T.astype(BF16)

        @pl.when(b + 2 < NB)
        def _():
            for copy in block_copies(b + 2):
                copy.start()

        @pl.when(b == 0)
        def _():
            wcopies[1].wait()
            wcopies[2].wait()

        @pl.when(b >= 2)
        def _():
            term_copy(b - 2).wait_send()

        for n in range(HALF // 256):
            t = dot(dgu[rows, :], wgu[pl.ds(pl.multiple_of((1 - c) * HALF + n * 256, 256), 256), :], NT)
            term_s[slot, :, n * 256:(n + 1) * 256] = t.astype(BF16)
        term_copy(b).start()
        for n in range(HALF // 256):
            t = dot(dgu[rows, :], wgu[pl.ds(pl.multiple_of(c * HALF + n * 256, 256), 256), :], NT)
            own[rows, n * 256:(n + 1) * 256] = t

    def dw_gate_up(i):
        slot = lax.rem(i, 2)
        tile_copy(x_hbm, i).wait()
        for j in range(M // 256):
            tile_t[:, j * 256:(j + 1) * 256] = tile[slot, j * 256:(j + 1) * 256, :].T

        @pl.when(i + 2 < NB)
        def _():
            tile_copy(x_hbm, i + 2).start()

        @pl.when(i + 2 >= NB)
        def _():
            tile_copy(dy_hbm, i + 2 - NB).start()

        rows = pl.ds(pl.multiple_of(i * TB, TB), TB)
        for n in range(F // 256):
            cols = slice(n * 256, (n + 1) * 256)
            dwg[rows, cols] = dot(tile_t[...], dgu[:, n * 256:(n + 1) * 256], NN).astype(BF16)
            dwu[rows, cols] = dot(tile_t[...], dgu[:, F + n * 256:F + (n + 1) * 256], NN).astype(BF16)

    def dw_down(i):
        slot = lax.rem(i, 2)
        tile_copy(dy_hbm, i).wait()

        cols = pl.ds(pl.multiple_of(i * TB, TB), TB)
        for n in range(F // 256):
            dwd[n * 256:(n + 1) * 256, cols] = dot(hid_t[n * 256:(n + 1) * 256, :], tile[slot], NN).astype(BF16)

        @pl.when(i + 2 < NB)
        def _():
            tile_copy(dy_hbm, i + 2).start()

    base = pl.multiple_of(c * HALF, HALF)
    side, off_side = root, 1 - root

    def rows_of(k, half=None):
        if half is None:
            return pl.ds(pl.multiple_of(k * R, R), R)
        return pl.ds(pl.multiple_of(k * R + half * H, H), H)

    def got(ref, k):
        return ref.at[pl.ds(pl.multiple_of(k * H, H), H), :]

    def pair(ref, k):
        return ref.at[pl.ds(pl.multiple_of(k // 2 * H, H), H), :]

    def whole(ref, k):
        return ref.at[pl.ds(pl.multiple_of(k // 2 * R, R), R), :]

    def final(k, half, col, width, core=None):
        start = pl.multiple_of((base if core is None else core) + col, 128)
        return fin.at[rows_of(k, half), pl.ds(start, width)]

    def message(kind, k, there=False):
        slot = lax.rem(k, NS)
        if kind in (A1, A2, A3):
            src, dst, peer = {A1: (sa1, ra1, across), A2: (sa2, ra2, near), A3: (sa3, ra3, far)}[kind]
            src, dst = src.at[slot], got(dst, k)
        elif kind == B1:
            src, dst, peer = sb1.at[slot], whole(rb1, k), near
        elif kind in (C1, B2, C2, B3, C3, C4):
            src, dst, peer = {
                C1: (sb2, rb4, near), B2: (sb2, rb2, far), C2: (sb2, rb2, far), B3: (sb3, rb3, across), C3: (sb3, rb3, near),
                C4: (sb4, rb4, across)}[kind]
            src, dst = src.at[slot], (got if kind in (B2, C2, B3, C3) else pair)(dst, k)
        elif kind in (FDA, FDB):
            core = pl.multiple_of((1 - c) * HALF if there else c * HALF, HALF)
            src = dst = final(k, None, *((0, WA) if kind == FDA else (WA, WB)), core=core)
            peer = mate
        else:
            mine, theirs, col, width, peer = {
                FAO: (y, y, 0, WA, near), FAY: (y, 1 - y, 0, WA, across),
                FBO: (side, side, WA, WB, near), FBI: (side, off_side, WA, WB, far), FB2: (off_side, off_side, WA, WB, near),
                FC1: (side, side, WA, WB, near), FC2: (side, off_side, WA, WB, far), FC3: (off_side, off_side, WA, WB, near),
            }[kind]
            src = dst = final(k, theirs if there else mine, col, width)
        row = ROW[kind]
        return pltpu.make_async_remote_copy(
            src, dst, send.at[row, slot], recv.at[row, k], device_id={"tp": peer}, device_id_type=MESH)

    def go(kind, k):
        message(kind, k).start()

    def free(kind, k):
        @pl.when(k >= NS)
        def _():
            message(kind, k - NS).wait_send()

    def pass_on(kind, k):
        free(kind, k)
        go(kind, k)

    def arrived(kind, k):
        message(kind, k, there=True).wait_recv()

    def mine_of(k, half, col, width):
        return own[rows_of(k, half), col:col + width]

    def with_mate(k, half, col, width):
        return mine_of(k, half, col, width) + term_r[rows_of(k, half), col:col + width].astype(F32)

    def keep(k, half, col, width, value):
        own[rows_of(k, half), col:col + width] = value

    def send_sum(kind, ref, k, value):
        free(kind, k)
        ref[lax.rem(k, NS)] = value.astype(BF16)
        go(kind, k)

    def put_final(k, half, col, width, sent, received):
        final(k, half, col, width)[...] = (sent[lax.rem(k, NS)].astype(F32) + received[...].astype(F32)).astype(BF16)

    on_inner, on_outer = pl.when(inner), pl.when(outer)

    def a1(k):
        @pl.when(lax.rem(k, TB // R) == 0)
        def _():
            term_copy(k // (TB // R)).wait_recv()

        send_sum(A1, sa1, k, with_mate(k, 1 - y, 0, WA))
        keep(k, y, 0, WA, with_mate(k, y, 0, WA))

    def a2(k):
        arrived(A1, k)

        @on_outer
        def _():
            send_sum(A2, sa2, k, mine_of(k, y, 0, WA) + got(ra1, k)[...].astype(F32))

        @on_inner
        def _():
            keep(k, y, 0, WA, mine_of(k, y, 0, WA) + got(ra1, k)[...].astype(F32))

    def a3(k):
        @on_inner
        def _():
            arrived(A2, k)
            send_sum(A3, sa3, k, mine_of(k, y, 0, WA) + got(ra2, k)[...].astype(F32))

    def a4(k):
        @on_inner
        def _():
            arrived(A3, k)
            put_final(k, y, 0, WA, sa3, got(ra3, k))
            pass_on(FAO, k)
            pass_on(FAY, k)

    def a5(k):
        @on_inner
        def _():
            arrived(FAY, k)
            pass_on(FDA, k)

        @on_outer
        def _():
            arrived(FAO, k)
            pass_on(FAY, k)

    def a6(k):
        @on_outer
        def _():
            arrived(FAY, k)
            pass_on(FDA, k)

    def b1(k):
        @on_outer
        def _():
            send_sum(B1, sb1, k, with_mate(k, None, WA, WB))

        @on_inner
        def _():
            keep(k, None, WA, WB, with_mate(k, None, WA, WB))

    def half_of(ref, k, half):
        return ref[pl.ds(pl.multiple_of(k // 2 * R + half * H, H), H), :].astype(F32)

    def b2(k):
        @on_inner
        def _():
            arrived(B1, k)
            send_sum(B2, sb2, k, mine_of(k, off_side, WA, WB) + half_of(rb1, k, off_side))
            keep(k, side, WA, WB, mine_of(k, side, WA, WB) + half_of(rb1, k, side))

    def b3(k):
        @on_inner
        def _():
            arrived(B2, k)
            send_sum(B3, sb3, k, mine_of(k, side, WA, WB) + got(rb2, k)[...].astype(F32))

    def b4(k):
        @on_inner
        def _():
            arrived(B3, k)
            put_final(k, side, WA, WB, sb3, got(rb3, k))
            pass_on(FBI, k)
            pass_on(FBO, k)

    def b5(k):
        @on_inner
        def _():
            arrived(FBI, k)
            pass_on(FB2, k)
            pass_on(FDB, k)

    def b6(k):
        @on_outer
        def _():
            arrived(FBO, k)
            arrived(FB2, k)
            pass_on(FDB, k)

    def c1(k):
        @on_outer
        def _():
            send_sum(C1, sb2, k, with_mate(k, off_side, WA, WB))
            keep(k, side, WA, WB, with_mate(k, side, WA, WB))

        @on_inner
        def _():
            keep(k, None, WA, WB, with_mate(k, None, WA, WB))

    def c2(k):
        @on_inner
        def _():
            arrived(C1, k)
            send_sum(C2, sb2, k, mine_of(k, off_side, WA, WB) + pair(rb4, k)[...].astype(F32))

    def c3(k):
        @on_inner
        def _():
            arrived(C2, k)
            send_sum(C3, sb3, k, mine_of(k, side, WA, WB) + got(rb2, k)[...].astype(F32))

    def c4(k):
        @on_outer
        def _():
            arrived(C3, k)
            send_sum(C4, sb4, k, mine_of(k, side, WA, WB) + got(rb3, k)[...].astype(F32))

    def c5(k):
        @on_outer
        def _():
            arrived(C4, k)
            put_final(k, side, WA, WB, sb4, pair(rb4, k))
            pass_on(FC1, k)

    def c6(k):
        @on_inner
        def _():
            arrived(FC1, k)
            pass_on(FC2, k)

    def c7(k):
        @on_inner
        def _():
            arrived(FC2, k)
            pass_on(FC3, k)
            pass_on(FDB, k)

    def c8(k):
        @on_outer
        def _():
            arrived(FC3, k)
            pass_on(FDB, k)

    events = (
        [(event, 0, at) for event, at in zip((b1, b2, b3, b4, b5, b6), B_AT)]
        + [(event, 1, at) for event, at in zip((c1, c2, c3, c4, c5, c6, c7, c8), C_AT)]
        + [(event, None, at) for event, at in zip((a1, a2, a3, a4, a5, a6), A_AT)]
    )
    events.sort(key=lambda entry: (entry[2], entry[0] is a1 and -1))
    steps = max(at for _, _, at in events) + S

    def step(s, _):
        for event, parity, offset in events:
            k = s - offset
            due = jnp.logical_and(k >= 0, k < S)
            if parity is not None:
                due = jnp.logical_and(due, lax.rem(k + S, 2) == parity)

            @pl.when(due)
            def _(event=event, k=k):
                event(k)

        @pl.when(jnp.logical_and(lax.rem(s, 2) == 0, s < 2 * NB))
        def _():
            terms(s // 2)

        @pl.when(jnp.logical_and(s >= 2 * NB, s < 3 * NB))
        def _():
            dw_gate_up(s - 2 * NB)

        @pl.when(jnp.logical_and(s >= 3 * NB, s < 4 * NB))
        def _():
            dw_down(s - 3 * NB)

        return 0

    lax.fori_loop(0, steps, step, 0)

    for b in (NB - 2, NB - 1):
        term_copy(b).wait_send()

    def landed(k, _):
        arrived(FDA, k)
        arrived(FDB, k)
        return 0

    lax.fori_loop(0, S, landed, 0)

    def drain(kinds, parity=None):
        for kind in kinds:
            for k in range(S - NS, S):
                if parity is None or k % 2 == parity:
                    message(kind, k).wait_send()

    drain((A1, FAY, FDA, FDB))

    @on_inner
    def _():
        drain((A3, FAO))
        drain((B2, B3, FBO, FBI, FB2), 0)
        drain((C2, C3, FC2, FC3), 1)

    @on_outer
    def _():
        drain((A2,))
        drain((B1,), 0)
        drain((C1, C4, FC1), 1)


PIECES = 4


def write_out(*refs):
    sources, targets, sems = refs[:4], refs[4:8], refs[8]
    copies = []
    for i, (source, target) in enumerate(zip(sources, targets)):
        size = source.shape[0] // PIECES
        for j in range(PIECES):
            rows = pl.ds(j * size, size)
            copies.append(pltpu.make_async_copy(source.at[rows, :], target.at[rows, :], sems.at[i, j]))
    for copy in copies:
        copy.start()
    for copy in copies:
        copy.wait()


def solution(mesh):
    def step(x, dy, gate, up, w_gate, w_up, w_down):
        vmem = pltpu.VMEM
        dma = pltpu.SemaphoreType.DMA
        scratch = [
            vmem((M, HALF), F32), vmem((M, HALF), BF16),
            *[vmem((M // 2, WA), BF16)] * 3,
            vmem((M // 2, WB), BF16), *[vmem((M // 2, WB), BF16)] * 2, vmem((M // 4, WB), BF16),
            vmem((2, TB, HALF), BF16),
            *[vmem((NS, H, WA), BF16)] * 3,
            vmem((NS, R, WB), BF16), *[vmem((NS, H, WB), BF16)] * 3,
            vmem((D, 2 * F), BF16), vmem((F, D), BF16),
            vmem((2, TB, D), BF16), vmem((2, TB, F), BF16), vmem((2, TB, F), BF16),
            vmem((M, 2 * F), BF16), vmem((F, M), BF16),
            vmem((2, M, TB), BF16), vmem((TB, M), BF16),
            dma((ROWS, NS)), dma((ROWS, S)), dma((2,)), dma((NB,)), dma((3,)), dma((2, 3)), dma((2,)),
        ]
        anywhere = pl.BlockSpec(memory_space=pl.ANY)
        shape = jax.ShapeDtypeStruct
        shapes = ((M, D), (D, F), (D, F), (F, D))
        grads = pl.pallas_call(
            kernel,
            out_shape=tuple(vmem(dims, BF16) for dims in shapes),
            in_specs=[anywhere] * 7,
            out_specs=(pl.BlockSpec(memory_space=vmem),) * 4,
            scratch_shapes=scratch,
            compiler_params=pltpu.CompilerParams(collective_id=0, has_side_effects=True, vmem_limit_bytes=LIMIT),
        )(x, dy, gate, up, w_gate, w_up, w_down)
        return pl.pallas_call(
            write_out,
            out_shape=tuple(shape(dims, BF16) for dims in shapes),
            in_specs=[pl.BlockSpec(memory_space=vmem)] * 4,
            out_specs=(anywhere,) * 4,
            scratch_shapes=[dma((4, PIECES))],
            compiler_params=pltpu.CompilerParams(vmem_limit_bytes=1 << 20),
        )(*grads)

    tokens, columns, rows = P("dp", None), P(None, "tp"), P("tp", None)
    return jax.shard_map(
        step,
        mesh=mesh,
        in_specs=(tokens, tokens, P("dp", "tp"), P("dp", "tp"), columns, columns, rows),
        out_specs=(tokens, P("dp", "tp"), P("dp", "tp"), P(("dp", "tp"), None)),
        check_vma=False,
    )
```

```python
import functools

import jax
import jax.numpy as jnp
from jax import lax
from jax.experimental import pallas as pl
from jax.experimental.pallas import tpu as pltpu
from jax.sharding import PartitionSpec as P

MESH = pl.DeviceIdType.MESH
F32, BF16 = jnp.float32, jnp.bfloat16

M, D, F = 2048, 2048, 512
HALF = D // 2
WA, WB = 640, 384
R = 64
H = R // 2
S = M // R
TB = 256
NB = M // TB
A_AT = (3, 6, 8, 10, 15, 20)
B_AT = (3, 5, 7, 10, 12, 18)
C_AT = (3, 5, 7, 9, 11, 13, 15, 25)
NS = 4
LIMIT = 48 * 1024 * 1024

A1, A2, A3, FAO, FAY, B1, B2, B3, FBO, FBI, FB2, C1, C2, C3, C4, FC1, FC2, FC3, FDA, FDB = range(20)
ROW = {kind: row for row, kinds in enumerate((
    (A1,), (A2,), (A3,), (FAO,), (FAY,), (B1, C1), (B2, C2), (B3, C3), (FBO, C4), (FBI, FC2), (FB2, FC3), (FC1,), (FDA,), (FDB,)
)) for kind in kinds}
ROWS = 14
NT = (((1,), (1,)), ((), ()))
NN = (((1,), (0,)), ((), ()))


def dot(a, b, dims):
    return lax.dot_general(a, b, dims, preferred_element_type=F32)


def kernel(x_hbm, dy_hbm, gate_hbm, up_hbm, wg_hbm, wu_hbm, wd_hbm, fin, dwg, dwu, dwd,
           own, term_r, ra1, ra2, ra3, rb1, rb2, rb3, rb4, term_s, sa1, sa2, sa3, sb1, sb2, sb3, sb4,
           wgu, wd, dyb, gb, ub, dgu, hid_t, tile, tile_t,
           send, recv, tsend, trecv, wsem, bsem, tilesem):
    me = lax.axis_index("tp")
    c, z, y = lax.rem(me, 2), lax.rem(me // 2, 4), me // 8
    at = lambda yy, zz, cc: (yy * 4 + zz) * 2 + cc
    mate = at(y, z, 1 - c)
    across = at(1 - y, z, c)
    inner = jnp.logical_or(z == 1, z == 2)
    outer = jnp.logical_not(inner)
    right_half = z // 2
    near = at(y, jnp.where(z == 0, 1, jnp.where(z == 1, 0, jnp.where(z == 2, 3, 2))), c)
    far = at(y, jnp.where(z == 1, 2, 1), c)
    root = right_half

    barrier = pltpu.get_barrier_semaphore()
    for peer in (mate, across, near):
        pl.semaphore_signal(barrier, inc=1, device_id={"tp": peer}, device_id_type=MESH)

    @pl.when(inner)
    def _():
        pl.semaphore_signal(barrier, inc=1, device_id={"tp": far}, device_id_type=MESH)

    wcopies = [
        pltpu.make_async_copy(wd_hbm, wd, wsem.at[0]),
        pltpu.make_async_copy(wg_hbm, wgu.at[:, pl.ds(0, F)], wsem.at[1]),
        pltpu.make_async_copy(wu_hbm, wgu.at[:, pl.ds(F, F)], wsem.at[2]),
    ]

    def block_copies(b):
        slot, rows = lax.rem(b, 2), pl.ds(b * TB, TB)
        return [
            pltpu.make_async_copy(dy_hbm.at[rows, :], dyb.at[slot], bsem.at[slot, 0]),
            pltpu.make_async_copy(gate_hbm.at[rows, :], gb.at[slot], bsem.at[slot, 1]),
            pltpu.make_async_copy(up_hbm.at[rows, :], ub.at[slot], bsem.at[slot, 2]),
        ]

    def tile_copy(ref, i):
        slot = 0 if ref is x_hbm else 1
        return pltpu.make_async_copy(ref.at[:, pl.ds(i * TB, TB)], tile.at[slot], tilesem.at[slot])

    wcopies[0].start()
    for copy in block_copies(0):
        copy.start()
    wcopies[1].start()
    wcopies[2].start()

    @pl.when(inner)
    def _():
        pl.semaphore_wait(barrier, 4)

    @pl.when(outer)
    def _():
        pl.semaphore_wait(barrier, 3)

    def term_copy(b):
        slot, rows = lax.rem(b, 2), pl.ds(b * TB, TB)
        return pltpu.make_async_remote_copy(
            term_s.at[slot], term_r.at[rows, :], tsend.at[slot], trecv.at[b],
            device_id={"tp": mate}, device_id_type=MESH)

    def hidden_grads(b):
        slot = lax.rem(b, 2)
        row = pl.multiple_of(b * TB, TB)
        rows = pl.ds(row, TB)

        @pl.when(b == 0)
        def _():
            wcopies[0].wait()

        for copy in block_copies(b):
            copy.wait()
        for n in range(F // 256):
            cols = slice(n * 256, (n + 1) * 256)
            dh = dot(dyb[slot], wd[cols, :], NT)
            g, u = gb[slot, :, cols].astype(F32), ub[slot, :, cols].astype(F32)
            sig = 1.0 / (1.0 + jnp.exp(-g))
            silu = g * sig
            du = dh * u
            dgu[rows, cols] = (du * sig + du * g * (sig * (1.0 - sig))).astype(BF16)
            dgu[rows, F + n * 256:F + (n + 1) * 256] = (dh * silu).astype(BF16)
            hid_t[cols, rows] = (silu * u).T.astype(BF16)

        @pl.when(b == 0)
        def _():
            for copy in block_copies(1):
                copy.start()

        @pl.when(b + 2 < NB)
        def _():
            for copy in block_copies(b + 2):
                copy.start()

        @pl.when(b == NB - 1)
        def _():
            tile_copy(x_hbm, 0).start()
            tile_copy(dy_hbm, 0).start()

    def terms_other(b):
        slot = lax.rem(b, 2)
        rows = pl.ds(pl.multiple_of(b * TB, TB), TB)

        @pl.when(b == 0)
        def _():
            wcopies[1].wait()
            wcopies[2].wait()

        @pl.when(b >= 2)
        def _():
            term_copy(b - 2).wait_send()

        for n in range(HALF // 256):
            t = dot(dgu[rows, :], wgu[pl.ds(pl.multiple_of((1 - c) * HALF + n * 256, 256), 256), :], NT)
            term_s[slot, :, n * 256:(n + 1) * 256] = t.astype(BF16)
        term_copy(b).start()

    def terms_own(b):
        rows = pl.ds(pl.multiple_of(b * TB, TB), TB)
        for n in range(HALF // 256):
            t = dot(dgu[rows, :], wgu[pl.ds(pl.multiple_of(c * HALF + n * 256, 256), 256), :], NT)
            own[rows, n * 256:(n + 1) * 256] = t

    def dw_gate(i):
        tile_copy(x_hbm, i).wait()
        for j in range(M // 256):
            tile_t[:, j * 256:(j + 1) * 256] = tile[0, j * 256:(j + 1) * 256, :].T

        @pl.when(i + 1 < NB)
        def _():
            tile_copy(x_hbm, i + 1).start()

        rows = pl.ds(pl.multiple_of(i * TB, TB), TB)
        for n in range(F // 256):
            dwg[rows, n * 256:(n + 1) * 256] = dot(tile_t[...], dgu[:, n * 256:(n + 1) * 256], NN).astype(BF16)

    def dw_up(i):
        rows = pl.ds(pl.multiple_of(i * TB, TB), TB)
        for n in range(F // 256):
            dwu[rows, n * 256:(n + 1) * 256] = dot(tile_t[...], dgu[:, F + n * 256:F + (n + 1) * 256], NN).astype(BF16)

    def dw_down(i):
        tile_copy(dy_hbm, i).wait()
        cols = pl.ds(pl.multiple_of(i * TB, TB), TB)
        for n in range(F // 256):
            dwd[n * 256:(n + 1) * 256, cols] = dot(hid_t[n * 256:(n + 1) * 256, :], tile[1], NN).astype(BF16)

        @pl.when(i + 1 < NB)
        def _():
            tile_copy(dy_hbm, i + 1).start()

    base = pl.multiple_of(c * HALF, HALF)
    side, off_side = root, 1 - root

    def rows_of(k, half=None):
        if half is None:
            return pl.ds(pl.multiple_of(k * R, R), R)
        return pl.ds(pl.multiple_of(k * R + half * H, H), H)

    def got(ref, k):
        return ref.at[pl.ds(pl.multiple_of(k * H, H), H), :]

    def pair(ref, k):
        return ref.at[pl.ds(pl.multiple_of(k // 2 * H, H), H), :]

    def whole(ref, k):
        return ref.at[pl.ds(pl.multiple_of(k // 2 * R, R), R), :]

    def final(k, half, col, width, core=None):
        start = pl.multiple_of((base if core is None else core) + col, 128)
        return fin.at[rows_of(k, half), pl.ds(start, width)]

    def message(kind, k, there=False):
        slot = lax.rem(k, NS)
        if kind in (A1, A2, A3):
            src, dst, peer = {A1: (sa1, ra1, across), A2: (sa2, ra2, near), A3: (sa3, ra3, far)}[kind]
            src, dst = src.at[slot], got(dst, k)
        elif kind == B1:
            src, dst, peer = sb1.at[slot], whole(rb1, k), near
        elif kind in (C1, B2, C2, B3, C3, C4):
            src, dst, peer = {
                C1: (sb2, rb4, near), B2: (sb2, rb2, far), C2: (sb2, rb2, far), B3: (sb3, rb3, across), C3: (sb3, rb3, near),
                C4: (sb4, rb4, across)}[kind]
            src, dst = src.at[slot], (got if kind in (B2, C2, B3, C3) else pair)(dst, k)
        elif kind in (FDA, FDB):
            core = pl.multiple_of((1 - c) * HALF if there else c * HALF, HALF)
            src = dst = final(k, None, *((0, WA) if kind == FDA else (WA, WB)), core=core)
            peer = mate
        else:
            mine, theirs, col, width, peer = {
                FAO: (y, y, 0, WA, near), FAY: (y, 1 - y, 0, WA, across),
                FBO: (side, side, WA, WB, near), FBI: (side, off_side, WA, WB, far), FB2: (off_side, off_side, WA, WB, near),
                FC1: (side, side, WA, WB, near), FC2: (side, off_side, WA, WB, far), FC3: (off_side, off_side, WA, WB, near),
            }[kind]
            src = dst = final(k, theirs if there else mine, col, width)
        row = ROW[kind]
        return pltpu.make_async_remote_copy(
            src, dst, send.at[row, slot], recv.at[row, k], device_id={"tp": peer}, device_id_type=MESH)

    def go(kind, k):
        message(kind, k).start()

    def free(kind, k):
        @pl.when(k >= NS)
        def _():
            message(kind, k - NS).wait_send()

    def pass_on(kind, k):
        free(kind, k)
        go(kind, k)

    def arrived(kind, k):
        message(kind, k, there=True).wait_recv()

    def mine_of(k, half, col, width):
        return own[rows_of(k, half), col:col + width]

    def with_mate(k, half, col, width):
        return mine_of(k, half, col, width) + term_r[rows_of(k, half), col:col + width].astype(F32)

    def keep(k, half, col, width, value):
        own[rows_of(k, half), col:col + width] = value

    def send_sum(kind, ref, k, value):
        free(kind, k)
        ref[lax.rem(k, NS)] = value.astype(BF16)
        go(kind, k)

    def put_final(k, half, col, width, sent, received):
        final(k, half, col, width)[...] = (sent[lax.rem(k, NS)].astype(F32) + received[...].astype(F32)).astype(BF16)

    on_inner, on_outer = pl.when(inner), pl.when(outer)

    def a1(k):
        @pl.when(lax.rem(k, TB // R) == 0)
        def _():
            term_copy(k // (TB // R)).wait_recv()

        send_sum(A1, sa1, k, with_mate(k, 1 - y, 0, WA))
        keep(k, y, 0, WA, with_mate(k, y, 0, WA))

    def a2(k):
        arrived(A1, k)

        @on_outer
        def _():
            send_sum(A2, sa2, k, mine_of(k, y, 0, WA) + got(ra1, k)[...].astype(F32))

        @on_inner
        def _():
            keep(k, y, 0, WA, mine_of(k, y, 0, WA) + got(ra1, k)[...].astype(F32))

    def a3(k):
        @on_inner
        def _():
            arrived(A2, k)
            send_sum(A3, sa3, k, mine_of(k, y, 0, WA) + got(ra2, k)[...].astype(F32))

    def a4(k):
        @on_inner
        def _():
            arrived(A3, k)
            put_final(k, y, 0, WA, sa3, got(ra3, k))
            pass_on(FAO, k)
            pass_on(FAY, k)

    def a5(k):
        @on_inner
        def _():
            arrived(FAY, k)
            pass_on(FDA, k)

        @on_outer
        def _():
            arrived(FAO, k)
            pass_on(FAY, k)

    def a6(k):
        @on_outer
        def _():
            arrived(FAY, k)
            pass_on(FDA, k)

    def b1(k):
        @on_outer
        def _():
            send_sum(B1, sb1, k, with_mate(k, None, WA, WB))

        @on_inner
        def _():
            keep(k, None, WA, WB, with_mate(k, None, WA, WB))

    def half_of(ref, k, half):
        return ref[pl.ds(pl.multiple_of(k // 2 * R + half * H, H), H), :].astype(F32)

    def b2(k):
        @on_inner
        def _():
            arrived(B1, k)
            send_sum(B2, sb2, k, mine_of(k, off_side, WA, WB) + half_of(rb1, k, off_side))
            keep(k, side, WA, WB, mine_of(k, side, WA, WB) + half_of(rb1, k, side))

    def b3(k):
        @on_inner
        def _():
            arrived(B2, k)
            send_sum(B3, sb3, k, mine_of(k, side, WA, WB) + got(rb2, k)[...].astype(F32))

    def b4(k):
        @on_inner
        def _():
            arrived(B3, k)
            put_final(k, side, WA, WB, sb3, got(rb3, k))
            pass_on(FBI, k)
            pass_on(FBO, k)

    def b5(k):
        @on_inner
        def _():
            arrived(FBI, k)
            pass_on(FB2, k)
            pass_on(FDB, k)

    def b6(k):
        @on_outer
        def _():
            arrived(FBO, k)
            arrived(FB2, k)
            pass_on(FDB, k)

    def c1(k):
        @on_outer
        def _():
            send_sum(C1, sb2, k, with_mate(k, off_side, WA, WB))
            keep(k, side, WA, WB, with_mate(k, side, WA, WB))

        @on_inner
        def _():
            keep(k, None, WA, WB, with_mate(k, None, WA, WB))

    def c2(k):
        @on_inner
        def _():
            arrived(C1, k)
            send_sum(C2, sb2, k, mine_of(k, off_side, WA, WB) + pair(rb4, k)[...].astype(F32))

    def c3(k):
        @on_inner
        def _():
            arrived(C2, k)
            send_sum(C3, sb3, k, mine_of(k, side, WA, WB) + got(rb2, k)[...].astype(F32))

    def c4(k):
        @on_outer
        def _():
            arrived(C3, k)
            send_sum(C4, sb4, k, mine_of(k, side, WA, WB) + got(rb3, k)[...].astype(F32))

    def c5(k):
        @on_outer
        def _():
            arrived(C4, k)
            put_final(k, side, WA, WB, sb4, pair(rb4, k))
            pass_on(FC1, k)

    def c6(k):
        @on_inner
        def _():
            arrived(FC1, k)
            pass_on(FC2, k)

    def c7(k):
        @on_inner
        def _():
            arrived(FC2, k)
            pass_on(FC3, k)
            pass_on(FDB, k)

    def c8(k):
        @on_outer
        def _():
            arrived(FC3, k)
            pass_on(FDB, k)

    events = (
        [(event, 0, at) for event, at in zip((b1, b2, b3, b4, b5, b6), B_AT)]
        + [(event, 1, at) for event, at in zip((c1, c2, c3, c4, c5, c6, c7, c8), C_AT)]
        + [(event, None, at) for event, at in zip((a1, a2, a3, a4, a5, a6), A_AT)]
    )
    events.sort(key=lambda entry: (entry[2], entry[0] is a1 and -1))
    steps = max(at for _, _, at in events) + S

    term_units = hidden_grads, terms_other, terms_own
    grad_units = dw_gate, dw_up, dw_down

    def step(s, _):
        for event, parity, offset in events:
            k = s - offset
            due = jnp.logical_and(k >= 0, k < S)
            if parity is not None:
                due = jnp.logical_and(due, lax.rem(k + S, 2) == parity)

            @pl.when(due)
            def _(event=event, k=k):
                event(k)

        for first, units in ((0, term_units), (len(term_units) * NB, grad_units)):
            for i, unit in enumerate(units):
                due = jnp.logical_and(s >= first, s < first + len(units) * NB)

                @pl.when(jnp.logical_and(due, lax.rem(s, len(units)) == (first + i) % len(units)))
                def _(unit=unit, first=first, n=len(units)):
                    unit((s - first) // n)

        return 0

    lax.fori_loop(0, steps, step, 0)

    for b in (NB - 2, NB - 1):
        term_copy(b).wait_send()

    def landed(k, _):
        arrived(FDA, k)
        arrived(FDB, k)
        return 0

    lax.fori_loop(0, S, landed, 0)

    def drain(kinds, parity=None):
        for kind in kinds:
            for k in range(S - NS, S):
                if parity is None or k % 2 == parity:
                    message(kind, k).wait_send()

    drain((A1, FAY, FDA, FDB))

    @on_inner
    def _():
        drain((A3, FAO))
        drain((B2, B3, FBO, FBI, FB2), 0)
        drain((C2, C3, FC2, FC3), 1)

    @on_outer
    def _():
        drain((A2,))
        drain((B1,), 0)
        drain((C1, C4, FC1), 1)


PIECES = 4


def write_out(*refs):
    sources, targets, sems = refs[:4], refs[4:8], refs[8]
    copies = []
    for i, (source, target) in enumerate(zip(sources, targets)):
        size = source.shape[0] // PIECES
        for j in range(PIECES):
            rows = pl.ds(j * size, size)
            copies.append(pltpu.make_async_copy(source.at[rows, :], target.at[rows, :], sems.at[i, j]))
    for copy in copies:
        copy.start()
    for copy in copies:
        copy.wait()


def solution(mesh):
    def step(x, dy, gate, up, w_gate, w_up, w_down):
        vmem = pltpu.VMEM
        dma = pltpu.SemaphoreType.DMA
        scratch = [
            vmem((M, HALF), F32), vmem((M, HALF), BF16),
            *[vmem((M // 2, WA), BF16)] * 3,
            vmem((M // 2, WB), BF16), *[vmem((M // 2, WB), BF16)] * 2, vmem((M // 4, WB), BF16),
            vmem((2, TB, HALF), BF16),
            *[vmem((NS, H, WA), BF16)] * 3,
            vmem((NS, R, WB), BF16), *[vmem((NS, H, WB), BF16)] * 3,
            vmem((D, 2 * F), BF16), vmem((F, D), BF16),
            vmem((2, TB, D), BF16), vmem((2, TB, F), BF16), vmem((2, TB, F), BF16),
            vmem((M, 2 * F), BF16), vmem((F, M), BF16),
            vmem((2, M, TB), BF16), vmem((TB, M), BF16),
            dma((ROWS, NS)), dma((ROWS, S)), dma((2,)), dma((NB,)), dma((3,)), dma((2, 3)), dma((2,)),
        ]
        anywhere = pl.BlockSpec(memory_space=pl.ANY)
        shape = jax.ShapeDtypeStruct
        shapes = ((M, D), (D, F), (D, F), (F, D))
        grads = pl.pallas_call(
            kernel,
            out_shape=tuple(vmem(dims, BF16) for dims in shapes),
            in_specs=[anywhere] * 7,
            out_specs=(pl.BlockSpec(memory_space=vmem),) * 4,
            scratch_shapes=scratch,
            compiler_params=pltpu.CompilerParams(collective_id=0, has_side_effects=True, vmem_limit_bytes=LIMIT),
        )(x, dy, gate, up, w_gate, w_up, w_down)
        return pl.pallas_call(
            write_out,
            out_shape=tuple(shape(dims, BF16) for dims in shapes),
            in_specs=[pl.BlockSpec(memory_space=vmem)] * 4,
            out_specs=(anywhere,) * 4,
            scratch_shapes=[dma((4, PIECES))],
            compiler_params=pltpu.CompilerParams(vmem_limit_bytes=1 << 20),
        )(*grads)

    tokens, columns, rows = P("dp", None), P(None, "tp"), P("tp", None)
    return jax.shard_map(
        step,
        mesh=mesh,
        in_specs=(tokens, tokens, P("dp", "tp"), P("dp", "tp"), columns, columns, rows),
        out_specs=(tokens, P("dp", "tp"), P("dp", "tp"), P(("dp", "tp"), None)),
        check_vma=False,
    )
```

```python
import functools

import jax
import jax.numpy as jnp
from jax import lax
from jax.experimental import pallas as pl
from jax.experimental.pallas import tpu as pltpu
from jax.sharding import PartitionSpec as P

MESH = pl.DeviceIdType.MESH
F32, BF16 = jnp.float32, jnp.bfloat16

M, D, F = 2048, 2048, 512
HALF = D // 2
WA, WB = 640, 384
R = 64
H = R // 2
S = M // R
TB = 256
NB = M // TB
A_AT = (3, 6, 8, 10, 14, 17)
B_AT = (3, 5, 7, 10, 12, 19)
C_AT = (3, 5, 7, 9, 11, 13, 15, 21)
NS = 4
LIMIT = 48 * 1024 * 1024

A1, A2, A3, FAO, FAY, B1, B2, B3, FBO, FBI, FB2, C1, C2, C3, C4, FC1, FC2, FC3, FDA, FDB = range(20)
ROW = {kind: row for row, kinds in enumerate((
    (A1,), (A2,), (A3,), (FAO,), (FAY,), (B1, C1), (B2, C2), (B3, C3), (FBO, C4), (FBI, FC2), (FB2, FC3), (FC1,), (FDA,), (FDB,)
)) for kind in kinds}
ROWS = 14
NT = (((1,), (1,)), ((), ()))
NN = (((1,), (0,)), ((), ()))


def dot(a, b, dims):
    return lax.dot_general(a, b, dims, preferred_element_type=F32)


def kernel(x_hbm, dy_hbm, gate_hbm, up_hbm, wg_hbm, wu_hbm, wd_hbm, fin, dwg, dwu, dwd,
           own, term_r, ra1, ra2, ra3, rb1, rb2, rb3, rb4, term_s, sa1, sa2, sa3, sb1, sb2, sb3, sb4,
           wgu, wd, dyb, gb, ub, dgu, hid_t, tile, tile_t,
           send, recv, tsend, trecv, wsem, bsem, tilesem):
    me = lax.axis_index("tp")
    c, z, y = lax.rem(me, 2), lax.rem(me // 2, 4), me // 8
    at = lambda yy, zz, cc: (yy * 4 + zz) * 2 + cc
    mate = at(y, z, 1 - c)
    across = at(1 - y, z, c)
    inner = jnp.logical_or(z == 1, z == 2)
    outer = jnp.logical_not(inner)
    right_half = z // 2
    near = at(y, jnp.where(z == 0, 1, jnp.where(z == 1, 0, jnp.where(z == 2, 3, 2))), c)
    far = at(y, jnp.where(z == 1, 2, 1), c)
    root = right_half

    barrier = pltpu.get_barrier_semaphore()
    for peer in (mate, across, near):
        pl.semaphore_signal(barrier, inc=1, device_id={"tp": peer}, device_id_type=MESH)

    @pl.when(inner)
    def _():
        pl.semaphore_signal(barrier, inc=1, device_id={"tp": far}, device_id_type=MESH)

    wcopies = [
        pltpu.make_async_copy(wd_hbm, wd, wsem.at[0]),
        pltpu.make_async_copy(wg_hbm, wgu.at[:, pl.ds(0, F)], wsem.at[1]),
        pltpu.make_async_copy(wu_hbm, wgu.at[:, pl.ds(F, F)], wsem.at[2]),
    ]

    def block_copies(b):
        slot, rows = lax.rem(b, 2), pl.ds(b * TB, TB)
        return [
            pltpu.make_async_copy(dy_hbm.at[rows, :], dyb.at[slot], bsem.at[slot, 0]),
            pltpu.make_async_copy(gate_hbm.at[rows, :], gb.at[slot], bsem.at[slot, 1]),
            pltpu.make_async_copy(up_hbm.at[rows, :], ub.at[slot], bsem.at[slot, 2]),
        ]

    def tile_copy(ref, i):
        slot = 0 if ref is x_hbm else 1
        return pltpu.make_async_copy(ref.at[:, pl.ds(i * TB, TB)], tile.at[slot], tilesem.at[slot])

    wcopies[0].start()
    for copy in block_copies(0):
        copy.start()
    wcopies[1].start()
    wcopies[2].start()

    @pl.when(inner)
    def _():
        pl.semaphore_wait(barrier, 4)

    @pl.when(outer)
    def _():
        pl.semaphore_wait(barrier, 3)

    def term_copy(b):
        slot, rows = lax.rem(b, 2), pl.ds(b * TB, TB)
        return pltpu.make_async_remote_copy(
            term_s.at[slot], term_r.at[rows, :], tsend.at[slot], trecv.at[b],
            device_id={"tp": mate}, device_id_type=MESH)

    def hidden_grads(b):
        slot = lax.rem(b, 2)
        row = pl.multiple_of(b * TB, TB)
        rows = pl.ds(row, TB)

        @pl.when(b == 0)
        def _():
            wcopies[0].wait()

        for copy in block_copies(b):
            copy.wait()
        for n in range(F // 256):
            cols = slice(n * 256, (n + 1) * 256)
            dh = dot(dyb[slot], wd[cols, :], NT)
            g, u = gb[slot, :, cols].astype(F32), ub[slot, :, cols].astype(F32)
            sig = 1.0 / (1.0 + jnp.exp(-g))
            silu = g * sig
            du = dh * u
            dgu[rows, cols] = (du * sig + du * g * (sig * (1.0 - sig))).astype(BF16)
            dgu[rows, F + n * 256:F + (n + 1) * 256] = (dh * silu).astype(BF16)
            hid_t[cols, rows] = (silu * u).T.astype(BF16)

        @pl.when(b == 0)
        def _():
            for copy in block_copies(1):
                copy.start()

        @pl.when(b + 2 < NB)
        def _():
            for copy in block_copies(b + 2):
                copy.start()

        @pl.when(b == NB - 1)
        def _():
            tile_copy(x_hbm, 0).start()
            tile_copy(dy_hbm, 0).start()

    def terms_other(b):
        slot = lax.rem(b, 2)
        rows = pl.ds(pl.multiple_of(b * TB, TB), TB)

        @pl.when(b == 0)
        def _():
            wcopies[1].wait()
            wcopies[2].wait()

        @pl.when(b >= 2)
        def _():
            term_copy(b - 2).wait_send()

        for n in range(HALF // 256):
            t = dot(dgu[rows, :], wgu[pl.ds(pl.multiple_of((1 - c) * HALF + n * 256, 256), 256), :], NT)
            term_s[slot, :, n * 256:(n + 1) * 256] = t.astype(BF16)
        term_copy(b).start()

    def terms_own(b):
        rows = pl.ds(pl.multiple_of(b * TB, TB), TB)
        for n in range(HALF // 256):
            t = dot(dgu[rows, :], wgu[pl.ds(pl.multiple_of(c * HALF + n * 256, 256), 256), :], NT)
            own[rows, n * 256:(n + 1) * 256] = t

    def dw_gate(i):
        tile_copy(x_hbm, i).wait()
        for j in range(M // 256):
            tile_t[:, j * 256:(j + 1) * 256] = tile[0, j * 256:(j + 1) * 256, :].T

        @pl.when(i + 1 < NB)
        def _():
            tile_copy(x_hbm, i + 1).start()

        rows = pl.ds(pl.multiple_of(i * TB, TB), TB)
        for n in range(F // 256):
            dwg[rows, n * 256:(n + 1) * 256] = dot(tile_t[...], dgu[:, n * 256:(n + 1) * 256], NN).astype(BF16)

    def dw_up(i):
        rows = pl.ds(pl.multiple_of(i * TB, TB), TB)
        for n in range(F // 256):
            dwu[rows, n * 256:(n + 1) * 256] = dot(tile_t[...], dgu[:, F + n * 256:F + (n + 1) * 256], NN).astype(BF16)

    def dw_down(i):
        tile_copy(dy_hbm, i).wait()
        cols = pl.ds(pl.multiple_of(i * TB, TB), TB)
        for n in range(F // 256):
            dwd[n * 256:(n + 1) * 256, cols] = dot(hid_t[n * 256:(n + 1) * 256, :], tile[1], NN).astype(BF16)

        @pl.when(i + 1 < NB)
        def _():
            tile_copy(dy_hbm, i + 1).start()

    base = pl.multiple_of(c * HALF, HALF)
    side, off_side = root, 1 - root

    def rows_of(k, half=None):
        if half is None:
            return pl.ds(pl.multiple_of(k * R, R), R)
        return pl.ds(pl.multiple_of(k * R + half * H, H), H)

    def got(ref, k):
        return ref.at[pl.ds(pl.multiple_of(k * H, H), H), :]

    def pair(ref, k):
        return ref.at[pl.ds(pl.multiple_of(k // 2 * H, H), H), :]

    def whole(ref, k):
        return ref.at[pl.ds(pl.multiple_of(k // 2 * R, R), R), :]

    def final(k, half, col, width, core=None):
        start = pl.multiple_of((base if core is None else core) + col, 128)
        return fin.at[rows_of(k, half), pl.ds(start, width)]

    def message(kind, k, there=False):
        slot = lax.rem(k, NS)
        if kind in (A1, A2, A3):
            src, dst, peer = {A1: (sa1, ra1, across), A2: (sa2, ra2, near), A3: (sa3, ra3, far)}[kind]
            src, dst = src.at[slot], got(dst, k)
        elif kind == B1:
            src, dst, peer = sb1.at[slot], whole(rb1, k), near
        elif kind in (C1, B2, C2, B3, C3, C4):
            src, dst, peer = {
                C1: (sb2, rb4, near), B2: (sb2, rb2, far), C2: (sb2, rb2, far), B3: (sb3, rb3, across), C3: (sb3, rb3, near),
                C4: (sb4, rb4, across)}[kind]
            src, dst = src.at[slot], (got if kind in (B2, C2, B3, C3) else pair)(dst, k)
        elif kind in (FDA, FDB):
            core = pl.multiple_of((1 - c) * HALF if there else c * HALF, HALF)
            src = dst = final(k, None, *((0, WA) if kind == FDA else (WA, WB)), core=core)
            peer = mate
        else:
            mine, theirs, col, width, peer = {
                FAO: (y, y, 0, WA, near), FAY: (y, 1 - y, 0, WA, across),
                FBO: (side, side, WA, WB, near), FBI: (side, off_side, WA, WB, far), FB2: (off_side, off_side, WA, WB, near),
                FC1: (side, side, WA, WB, near), FC2: (side, off_side, WA, WB, far), FC3: (off_side, off_side, WA, WB, near),
            }[kind]
            src = dst = final(k, theirs if there else mine, col, width)
        row = ROW[kind]
        return pltpu.make_async_remote_copy(
            src, dst, send.at[row, slot], recv.at[row, k], device_id={"tp": peer}, device_id_type=MESH)

    def go(kind, k):
        message(kind, k).start()

    def free(kind, k):
        @pl.when(k >= NS)
        def _():
            message(kind, k - NS).wait_send()

    def pass_on(kind, k):
        free(kind, k)
        go(kind, k)

    def arrived(kind, k):
        message(kind, k, there=True).wait_recv()

    def mine_of(k, half, col, width):
        return own[rows_of(k, half), col:col + width]

    def with_mate(k, half, col, width):
        return mine_of(k, half, col, width) + term_r[rows_of(k, half), col:col + width].astype(F32)

    def keep(k, half, col, width, value):
        own[rows_of(k, half), col:col + width] = value

    def send_sum(kind, ref, k, value):
        free(kind, k)
        ref[lax.rem(k, NS)] = value.astype(BF16)
        go(kind, k)

    def put_final(k, half, col, width, sent, received):
        final(k, half, col, width)[...] = (sent[lax.rem(k, NS)].astype(F32) + received[...].astype(F32)).astype(BF16)

    on_inner, on_outer = pl.when(inner), pl.when(outer)

    def a1(k):
        @pl.when(lax.rem(k, TB // R) == 0)
        def _():
            term_copy(k // (TB // R)).wait_recv()

        send_sum(A1, sa1, k, with_mate(k, 1 - y, 0, WA))
        keep(k, y, 0, WA, with_mate(k, y, 0, WA))

    def a2(k):
        arrived(A1, k)

        @on_outer
        def _():
            send_sum(A2, sa2, k, mine_of(k, y, 0, WA) + got(ra1, k)[...].astype(F32))

        @on_inner
        def _():
            keep(k, y, 0, WA, mine_of(k, y, 0, WA) + got(ra1, k)[...].astype(F32))

    def a3(k):
        @on_inner
        def _():
            arrived(A2, k)
            send_sum(A3, sa3, k, mine_of(k, y, 0, WA) + got(ra2, k)[...].astype(F32))

    def a4(k):
        @on_inner
        def _():
            arrived(A3, k)
            put_final(k, y, 0, WA, sa3, got(ra3, k))
            pass_on(FAO, k)
            pass_on(FAY, k)

    def a5(k):
        @on_inner
        def _():
            arrived(FAY, k)
            pass_on(FDA, k)

        @on_outer
        def _():
            arrived(FAO, k)
            pass_on(FAY, k)

    def a6(k):
        @on_outer
        def _():
            arrived(FAY, k)
            pass_on(FDA, k)

    def b1(k):
        @on_outer
        def _():
            send_sum(B1, sb1, k, with_mate(k, None, WA, WB))

        @on_inner
        def _():
            keep(k, None, WA, WB, with_mate(k, None, WA, WB))

    def half_of(ref, k, half):
        return ref[pl.ds(pl.multiple_of(k // 2 * R + half * H, H), H), :].astype(F32)

    def b2(k):
        @on_inner
        def _():
            arrived(B1, k)
            send_sum(B2, sb2, k, mine_of(k, off_side, WA, WB) + half_of(rb1, k, off_side))
            keep(k, side, WA, WB, mine_of(k, side, WA, WB) + half_of(rb1, k, side))

    def b3(k):
        @on_inner
        def _():
            arrived(B2, k)
            send_sum(B3, sb3, k, mine_of(k, side, WA, WB) + got(rb2, k)[...].astype(F32))

    def b4(k):
        @on_inner
        def _():
            arrived(B3, k)
            put_final(k, side, WA, WB, sb3, got(rb3, k))
            pass_on(FBI, k)
            pass_on(FBO, k)

    def b5(k):
        @on_inner
        def _():
            arrived(FBI, k)
            pass_on(FB2, k)
            pass_on(FDB, k)

    def b6(k):
        @on_outer
        def _():
            arrived(FBO, k)
            arrived(FB2, k)
            pass_on(FDB, k)

    def c1(k):
        @on_outer
        def _():
            send_sum(C1, sb2, k, with_mate(k, off_side, WA, WB))
            keep(k, side, WA, WB, with_mate(k, side, WA, WB))

        @on_inner
        def _():
            keep(k, None, WA, WB, with_mate(k, None, WA, WB))

    def c2(k):
        @on_inner
        def _():
            arrived(C1, k)
            send_sum(C2, sb2, k, mine_of(k, off_side, WA, WB) + pair(rb4, k)[...].astype(F32))

    def c3(k):
        @on_inner
        def _():
            arrived(C2, k)
            send_sum(C3, sb3, k, mine_of(k, side, WA, WB) + got(rb2, k)[...].astype(F32))

    def c4(k):
        @on_outer
        def _():
            arrived(C3, k)
            send_sum(C4, sb4, k, mine_of(k, side, WA, WB) + got(rb3, k)[...].astype(F32))

    def c5(k):
        @on_outer
        def _():
            arrived(C4, k)
            put_final(k, side, WA, WB, sb4, pair(rb4, k))
            pass_on(FC1, k)

    def c6(k):
        @on_inner
        def _():
            arrived(FC1, k)
            pass_on(FC2, k)

    def c7(k):
        @on_inner
        def _():
            arrived(FC2, k)
            pass_on(FC3, k)
            pass_on(FDB, k)

    def c8(k):
        @on_outer
        def _():
            arrived(FC3, k)
            pass_on(FDB, k)

    events = (
        [(event, 1, at) for event, at in zip((b1, b2, b3, b4, b5, b6), B_AT)]
        + [(event, 0, at) for event, at in zip((c1, c2, c3, c4, c5, c6, c7, c8), C_AT)]
        + [(event, None, at) for event, at in zip((a1, a2, a3, a4, a5, a6), A_AT)]
    )
    order = (c2, c3, a1, c8, b3, b1, c4, b2, c1, a2, b6, a3, a4, c5, a6, b4, c6, a5, b5, c7)
    events.sort(key=lambda entry: order.index(entry[0]))
    steps = max(at for _, _, at in events) + S

    term_units = hidden_grads, terms_other, terms_own
    grad_units = dw_gate, dw_up, dw_down

    def step(s, _):
        for event, parity, offset in events:
            k = s - offset
            due = jnp.logical_and(k >= 0, k < S)
            if parity is not None:
                due = jnp.logical_and(due, lax.rem(k + S, 2) == parity)

            @pl.when(due)
            def _(event=event, k=k):
                event(k)

        for first, units in ((0, term_units), (len(term_units) * NB, grad_units)):
            for i, unit in enumerate(units):
                due = jnp.logical_and(s >= first, s < first + len(units) * NB)

                @pl.when(jnp.logical_and(due, lax.rem(s, len(units)) == (first + i) % len(units)))
                def _(unit=unit, first=first, n=len(units)):
                    unit((s - first) // n)

        return 0

    lax.fori_loop(0, steps, step, 0)

    for b in (NB - 2, NB - 1):
        term_copy(b).wait_send()

    def landed(k, _):
        arrived(FDA, k)
        arrived(FDB, k)
        return 0

    lax.fori_loop(0, S, landed, 0)

    def drain(kinds, parity=None):
        for kind in kinds:
            for k in range(S - NS, S):
                if parity is None or k % 2 == parity:
                    message(kind, k).wait_send()

    drain((A1, FAY, FDA, FDB))

    @on_inner
    def _():
        drain((A3, FAO))
        drain((B2, B3, FBO, FBI, FB2), 1)
        drain((C2, C3, FC2, FC3), 0)

    @on_outer
    def _():
        drain((A2,))
        drain((B1,), 1)
        drain((C1, C4, FC1), 0)


PIECES = 4


def write_out(*refs):
    sources, targets, sems = refs[:4], refs[4:8], refs[8]
    copies = []
    for i, (source, target) in enumerate(zip(sources, targets)):
        size = source.shape[0] // PIECES
        for j in range(PIECES):
            rows = pl.ds(j * size, size)
            copies.append(pltpu.make_async_copy(source.at[rows, :], target.at[rows, :], sems.at[i, j]))
    for copy in copies:
        copy.start()
    for copy in copies:
        copy.wait()


def solution(mesh):
    def step(x, dy, gate, up, w_gate, w_up, w_down):
        vmem = pltpu.VMEM
        dma = pltpu.SemaphoreType.DMA
        scratch = [
            vmem((M, HALF), F32), vmem((M, HALF), BF16),
            *[vmem((M // 2, WA), BF16)] * 3,
            vmem((M // 2, WB), BF16), *[vmem((M // 2, WB), BF16)] * 2, vmem((M // 4, WB), BF16),
            vmem((2, TB, HALF), BF16),
            *[vmem((NS, H, WA), BF16)] * 3,
            vmem((NS, R, WB), BF16), *[vmem((NS, H, WB), BF16)] * 3,
            vmem((D, 2 * F), BF16), vmem((F, D), BF16),
            vmem((2, TB, D), BF16), vmem((2, TB, F), BF16), vmem((2, TB, F), BF16),
            vmem((M, 2 * F), BF16), vmem((F, M), BF16),
            vmem((2, M, TB), BF16), vmem((TB, M), BF16),
            dma((ROWS, NS)), dma((ROWS, S)), dma((2,)), dma((NB,)), dma((3,)), dma((2, 3)), dma((2,)),
        ]
        anywhere = pl.BlockSpec(memory_space=pl.ANY)
        shape = jax.ShapeDtypeStruct
        shapes = ((M, D), (D, F), (D, F), (F, D))
        grads = pl.pallas_call(
            kernel,
            out_shape=tuple(vmem(dims, BF16) for dims in shapes),
            in_specs=[anywhere] * 7,
            out_specs=(pl.BlockSpec(memory_space=vmem),) * 4,
            scratch_shapes=scratch,
            compiler_params=pltpu.CompilerParams(collective_id=0, has_side_effects=True, vmem_limit_bytes=LIMIT),
        )(x, dy, gate, up, w_gate, w_up, w_down)
        return pl.pallas_call(
            write_out,
            out_shape=tuple(shape(dims, BF16) for dims in shapes),
            in_specs=[pl.BlockSpec(memory_space=vmem)] * 4,
            out_specs=(anywhere,) * 4,
            scratch_shapes=[dma((4, PIECES))],
            compiler_params=pltpu.CompilerParams(vmem_limit_bytes=1 << 20),
        )(*grads)

    tokens, columns, rows = P("dp", None), P(None, "tp"), P("tp", None)
    return jax.shard_map(
        step,
        mesh=mesh,
        in_specs=(tokens, tokens, P("dp", "tp"), P("dp", "tp"), columns, columns, rows),
        out_specs=(tokens, P("dp", "tp"), P("dp", "tp"), P(("dp", "tp"), None)),
        check_vma=False,
    )
```

```python
import functools

import jax
import jax.numpy as jnp
from jax import lax
from jax.experimental import pallas as pl
from jax.experimental.pallas import tpu as pltpu
from jax.sharding import PartitionSpec as P

MESH = pl.DeviceIdType.MESH
F32, BF16 = jnp.float32, jnp.bfloat16

M, D, F = 2048, 2048, 512
HALF = D // 2
WA, WB = 640, 384
R = 64
H = R // 2
S = M // R
TB = 256
NB = M // TB
A_AT = (3, 6, 8, 10, 14, 17)
B_AT = (3, 5, 7, 10, 12, 19)
C_AT = (3, 5, 7, 9, 11, 13, 15, 21)
NS = 4
LIMIT = 48 * 1024 * 1024

A1, A2, A3, FAO, FAY, B1, B2, B3, FBO, FBI, FB2, C1, C2, C3, C4, FC1, FC2, FC3, FDA, FDB = range(20)
ROW = {kind: row for row, kinds in enumerate((
    (A1,), (A2,), (A3,), (FAO,), (FAY,), (B1, C1), (B2, C2), (B3, C3), (FBO, C4), (FBI, FC2), (FB2, FC3), (FC1,), (FDA,), (FDB,)
)) for kind in kinds}
ROWS = 14
NT = (((1,), (1,)), ((), ()))
NN = (((1,), (0,)), ((), ()))


def dot(a, b, dims):
    return lax.dot_general(a, b, dims, preferred_element_type=F32)


def kernel(x_hbm, dy_hbm, gate_hbm, up_hbm, wg_hbm, wu_hbm, wd_hbm, fin, dwg, dwu, dwd,
           own, term_r, ra1, ra2, ra3, rb1, rb2, rb3, rb4, term_s, sa1, sa2, sa3, sb1, sb2, sb3, sb4,
           wgu, wd, dyb, gb, ub, dgu, hid_t, tile, tile_t,
           send, recv, tsend, trecv, wsem, bsem, tilesem):
    me = lax.axis_index("tp")
    c, z, y = lax.rem(me, 2), lax.rem(me // 2, 4), me // 8
    at = lambda yy, zz, cc: (yy * 4 + zz) * 2 + cc
    mate = at(y, z, 1 - c)
    across = at(1 - y, z, c)
    inner = jnp.logical_or(z == 1, z == 2)
    outer = jnp.logical_not(inner)
    right_half = z // 2
    near = at(y, jnp.where(z == 0, 1, jnp.where(z == 1, 0, jnp.where(z == 2, 3, 2))), c)
    far = at(y, jnp.where(z == 1, 2, 1), c)
    root = right_half

    barrier = pltpu.get_barrier_semaphore()
    for peer in (mate, across, near):
        pl.semaphore_signal(barrier, inc=1, device_id={"tp": peer}, device_id_type=MESH)

    @pl.when(inner)
    def _():
        pl.semaphore_signal(barrier, inc=1, device_id={"tp": far}, device_id_type=MESH)

    wcopies = [
        pltpu.make_async_copy(wd_hbm, wd, wsem.at[0]),
        pltpu.make_async_copy(wg_hbm, wgu.at[:, pl.ds(0, F)], wsem.at[1]),
        pltpu.make_async_copy(wu_hbm, wgu.at[:, pl.ds(F, F)], wsem.at[2]),
    ]

    def block_copies(b):
        slot, rows = lax.rem(b, 2), pl.ds(b * TB, TB)
        return [
            pltpu.make_async_copy(dy_hbm.at[rows, :], dyb.at[slot], bsem.at[slot, 0]),
            pltpu.make_async_copy(gate_hbm.at[rows, :], gb.at[slot], bsem.at[slot, 1]),
            pltpu.make_async_copy(up_hbm.at[rows, :], ub.at[slot], bsem.at[slot, 2]),
        ]

    def tile_copy(ref, i):
        slot = 0 if ref is x_hbm else 1
        return pltpu.make_async_copy(ref.at[:, pl.ds(i * TB, TB)], tile.at[slot], tilesem.at[slot])

    wcopies[0].start()
    for copy in block_copies(0):
        copy.start()
    wcopies[1].start()
    wcopies[2].start()

    @pl.when(inner)
    def _():
        pl.semaphore_wait(barrier, 4)

    @pl.when(outer)
    def _():
        pl.semaphore_wait(barrier, 3)

    def term_copy(b):
        slot, rows = lax.rem(b, 2), pl.ds(b * TB, TB)
        return pltpu.make_async_remote_copy(
            term_s.at[slot], term_r.at[rows, :], tsend.at[slot], trecv.at[b],
            device_id={"tp": mate}, device_id_type=MESH)

    def hidden_grads(b):
        slot = lax.rem(b, 2)
        row = pl.multiple_of(b * TB, TB)
        rows = pl.ds(row, TB)

        @pl.when(b == 0)
        def _():
            wcopies[0].wait()

        for copy in block_copies(b):
            copy.wait()
        for n in range(F // 256):
            cols = slice(n * 256, (n + 1) * 256)
            dh = dot(dyb[slot], wd[cols, :], NT)
            g, u = gb[slot, :, cols].astype(F32), ub[slot, :, cols].astype(F32)
            sig = 1.0 / (1.0 + jnp.exp(-g))
            silu = g * sig
            du = dh * u
            dgu[rows, cols] = (du * sig + du * g * (sig * (1.0 - sig))).astype(BF16)
            dgu[rows, F + n * 256:F + (n + 1) * 256] = (dh * silu).astype(BF16)
            hid_t[cols, rows] = (silu * u).T.astype(BF16)

        @pl.when(b == 0)
        def _():
            for copy in block_copies(1):
                copy.start()

        @pl.when(b + 2 < NB)
        def _():
            for copy in block_copies(b + 2):
                copy.start()

        @pl.when(b == NB - 1)
        def _():
            tile_copy(x_hbm, 0).start()
            tile_copy(dy_hbm, 0).start()

    def terms_other(b):
        slot = lax.rem(b, 2)
        rows = pl.ds(pl.multiple_of(b * TB, TB), TB)

        @pl.when(b == 0)
        def _():
            wcopies[1].wait()
            wcopies[2].wait()

        @pl.when(b >= 2)
        def _():
            term_copy(b - 2).wait_send()

        for n in range(HALF // 256):
            t = dot(dgu[rows, :], wgu[pl.ds(pl.multiple_of((1 - c) * HALF + n * 256, 256), 256), :], NT)
            term_s[slot, :, n * 256:(n + 1) * 256] = t.astype(BF16)
        term_copy(b).start()

    def terms_own(b):
        rows = pl.ds(pl.multiple_of(b * TB, TB), TB)
        for n in range(HALF // 256):
            t = dot(dgu[rows, :], wgu[pl.ds(pl.multiple_of(c * HALF + n * 256, 256), 256), :], NT)
            own[rows, n * 256:(n + 1) * 256] = t

    def dw_gate(i):
        tile_copy(x_hbm, i).wait()
        for j in range(M // 256):
            tile_t[:, j * 256:(j + 1) * 256] = tile[0, j * 256:(j + 1) * 256, :].T

        @pl.when(i + 1 < NB)
        def _():
            tile_copy(x_hbm, i + 1).start()

        rows = pl.ds(pl.multiple_of(i * TB, TB), TB)
        for n in range(F // 256):
            dwg[rows, n * 256:(n + 1) * 256] = dot(tile_t[...], dgu[:, n * 256:(n + 1) * 256], NN).astype(BF16)

    def dw_up(i):
        rows = pl.ds(pl.multiple_of(i * TB, TB), TB)
        for n in range(F // 256):
            dwu[rows, n * 256:(n + 1) * 256] = dot(tile_t[...], dgu[:, F + n * 256:F + (n + 1) * 256], NN).astype(BF16)

    def dw_down(i):
        tile_copy(dy_hbm, i).wait()
        cols = pl.ds(pl.multiple_of(i * TB, TB), TB)
        for n in range(F // 256):
            dwd[n * 256:(n + 1) * 256, cols] = dot(hid_t[n * 256:(n + 1) * 256, :], tile[1], NN).astype(BF16)

        @pl.when(i + 1 < NB)
        def _():
            tile_copy(dy_hbm, i + 1).start()

    base = pl.multiple_of(c * HALF, HALF)
    side, off_side = root, 1 - root

    def rows_of(k, half=None):
        if half is None:
            return pl.ds(pl.multiple_of(k * R, R), R)
        return pl.ds(pl.multiple_of(k * R + half * H, H), H)

    def got(ref, k):
        return ref.at[pl.ds(pl.multiple_of(k * H, H), H), :]

    def pair(ref, k):
        return ref.at[pl.ds(pl.multiple_of(k // 2 * H, H), H), :]

    def whole(ref, k):
        return ref.at[pl.ds(pl.multiple_of(k // 2 * R, R), R), :]

    def final(k, half, col, width, core=None):
        start = pl.multiple_of((base if core is None else core) + col, 128)
        return fin.at[rows_of(k, half), pl.ds(start, width)]

    def message(kind, k, there=False):
        slot = lax.rem(k, NS)
        if kind in (A1, A2, A3):
            src, dst, peer = {A1: (sa1, ra1, across), A2: (sa2, ra2, near), A3: (sa3, ra3, far)}[kind]
            src, dst = src.at[slot], got(dst, k)
        elif kind == B1:
            src, dst, peer = sb1.at[slot], whole(rb1, k), near
        elif kind in (C1, B2, C2, B3, C3, C4):
            src, dst, peer = {
                C1: (sb2, rb4, near), B2: (sb2, rb2, far), C2: (sb2, rb2, far), B3: (sb3, rb3, across), C3: (sb3, rb3, near),
                C4: (sb4, rb4, across)}[kind]
            src, dst = src.at[slot], (got if kind in (B2, C2, B3, C3) else pair)(dst, k)
        elif kind in (FDA, FDB):
            core = pl.multiple_of((1 - c) * HALF if there else c * HALF, HALF)
            src = dst = final(k, None, *((0, WA) if kind == FDA else (WA, WB)), core=core)
            peer = mate
        else:
            mine, theirs, col, width, peer = {
                FAO: (y, y, 0, WA, near), FAY: (y, 1 - y, 0, WA, across),
                FBO: (side, side, WA, WB, near), FBI: (side, off_side, WA, WB, far), FB2: (off_side, off_side, WA, WB, near),
                FC1: (side, side, WA, WB, near), FC2: (side, off_side, WA, WB, far), FC3: (off_side, off_side, WA, WB, near),
            }[kind]
            src = dst = final(k, theirs if there else mine, col, width)
        row = ROW[kind]
        return pltpu.make_async_remote_copy(
            src, dst, send.at[row, slot], recv.at[row, k], device_id={"tp": peer}, device_id_type=MESH)

    def go(kind, k):
        message(kind, k).start()

    def free(kind, k):
        @pl.when(k >= NS)
        def _():
            message(kind, k - NS).wait_send()

    def pass_on(kind, k):
        free(kind, k)
        go(kind, k)

    def arrived(kind, k):
        message(kind, k, there=True).wait_recv()

    def mine_of(k, half, col, width):
        return own[rows_of(k, half), col:col + width]

    def with_mate(k, half, col, width):
        return mine_of(k, half, col, width) + term_r[rows_of(k, half), col:col + width].astype(F32)

    def keep(k, half, col, width, value):
        own[rows_of(k, half), col:col + width] = value

    def send_sum(kind, ref, k, value):
        free(kind, k)
        ref[lax.rem(k, NS)] = value.astype(BF16)
        go(kind, k)

    def put_final(k, half, col, width, sent, received):
        final(k, half, col, width)[...] = (sent[lax.rem(k, NS)].astype(F32) + received[...].astype(F32)).astype(BF16)

    on_inner, on_outer = pl.when(inner), pl.when(outer)

    def a1(k):
        @pl.when(lax.rem(k, TB // R) == 0)
        def _():
            term_copy(k // (TB // R)).wait_recv()

        send_sum(A1, sa1, k, with_mate(k, 1 - y, 0, WA))
        keep(k, y, 0, WA, with_mate(k, y, 0, WA))

    def a2(k):
        arrived(A1, k)

        @on_outer
        def _():
            send_sum(A2, sa2, k, mine_of(k, y, 0, WA) + got(ra1, k)[...].astype(F32))

        @on_inner
        def _():
            keep(k, y, 0, WA, mine_of(k, y, 0, WA) + got(ra1, k)[...].astype(F32))

    def a3(k):
        @on_inner
        def _():
            arrived(A2, k)
            send_sum(A3, sa3, k, mine_of(k, y, 0, WA) + got(ra2, k)[...].astype(F32))

    def a4(k):
        @on_inner
        def _():
            arrived(A3, k)
            put_final(k, y, 0, WA, sa3, got(ra3, k))
            pass_on(FAO, k)
            pass_on(FAY, k)

    def a5(k):
        @on_inner
        def _():
            arrived(FAY, k)
            pass_on(FDA, k)

        @on_outer
        def _():
            arrived(FAO, k)
            pass_on(FAY, k)

    def a6(k):
        @on_outer
        def _():
            arrived(FAY, k)
            pass_on(FDA, k)

    def b1(k):
        @on_outer
        def _():
            send_sum(B1, sb1, k, with_mate(k, None, WA, WB))

        @on_inner
        def _():
            keep(k, None, WA, WB, with_mate(k, None, WA, WB))

    def half_of(ref, k, half):
        return ref[pl.ds(pl.multiple_of(k // 2 * R + half * H, H), H), :].astype(F32)

    def b2(k):
        @on_inner
        def _():
            arrived(B1, k)
            send_sum(B2, sb2, k, mine_of(k, off_side, WA, WB) + half_of(rb1, k, off_side))
            keep(k, side, WA, WB, mine_of(k, side, WA, WB) + half_of(rb1, k, side))

    def b3(k):
        @on_inner
        def _():
            arrived(B2, k)
            send_sum(B3, sb3, k, mine_of(k, side, WA, WB) + got(rb2, k)[...].astype(F32))

    def b4(k):
        @on_inner
        def _():
            arrived(B3, k)
            put_final(k, side, WA, WB, sb3, got(rb3, k))
            pass_on(FBI, k)
            pass_on(FBO, k)

    def b5(k):
        @on_inner
        def _():
            arrived(FBI, k)
            pass_on(FB2, k)
            pass_on(FDB, k)

    def b6(k):
        @on_outer
        def _():
            arrived(FBO, k)
            arrived(FB2, k)
            pass_on(FDB, k)

    def c1(k):
        @on_outer
        def _():
            send_sum(C1, sb2, k, with_mate(k, off_side, WA, WB))
            keep(k, side, WA, WB, with_mate(k, side, WA, WB))

        @on_inner
        def _():
            keep(k, None, WA, WB, with_mate(k, None, WA, WB))

    def c2(k):
        @on_inner
        def _():
            arrived(C1, k)
            send_sum(C2, sb2, k, mine_of(k, off_side, WA, WB) + pair(rb4, k)[...].astype(F32))

    def c3(k):
        @on_inner
        def _():
            arrived(C2, k)
            send_sum(C3, sb3, k, mine_of(k, side, WA, WB) + got(rb2, k)[...].astype(F32))

    def c4(k):
        @on_outer
        def _():
            arrived(C3, k)
            send_sum(C4, sb4, k, mine_of(k, side, WA, WB) + got(rb3, k)[...].astype(F32))

    def c5(k):
        @on_outer
        def _():
            arrived(C4, k)
            put_final(k, side, WA, WB, sb4, pair(rb4, k))
            pass_on(FC1, k)

    def c6(k):
        @on_inner
        def _():
            arrived(FC1, k)
            pass_on(FC2, k)

    def c7(k):
        @on_inner
        def _():
            arrived(FC2, k)
            pass_on(FC3, k)
            pass_on(FDB, k)

    def c8(k):
        @on_outer
        def _():
            arrived(FC3, k)
            pass_on(FDB, k)

    events = (
        [(event, 1, at) for event, at in zip((b1, b2, b3, b4, b5, b6), B_AT)]
        + [(event, 0, at) for event, at in zip((c1, c2, c3, c4, c5, c6, c7, c8), C_AT)]
        + [(event, None, at) for event, at in zip((a1, a2, a3, a4, a5, a6), A_AT)]
    )
    order = (a1, c2, c3, b2, b3, c4, c1, b1, a2, a3, c5, a4, b4, c6, a5, b5, c7, c8, b6, a6)
    events.sort(key=lambda entry: order.index(entry[0]))
    steps = max(at for _, _, at in events) + S

    term_units = hidden_grads, terms_other, terms_own
    grad_units = dw_gate, dw_up, dw_down

    def step(s, _):
        for event, parity, offset in events:
            k = s - offset
            due = jnp.logical_and(k >= 0, k < S)
            if parity is not None:
                due = jnp.logical_and(due, lax.rem(k + S, 2) == parity)

            @pl.when(due)
            def _(event=event, k=k):
                event(k)

        for first, units in ((0, term_units), (len(term_units) * NB, grad_units)):
            for i, unit in enumerate(units):
                due = jnp.logical_and(s >= first, s < first + len(units) * NB)

                @pl.when(jnp.logical_and(due, lax.rem(s, len(units)) == (first + i) % len(units)))
                def _(unit=unit, first=first, n=len(units)):
                    unit((s - first) // n)

        return 0

    lax.fori_loop(0, steps, step, 0)

    for b in (NB - 2, NB - 1):
        term_copy(b).wait_send()

    def landed(k, _):
        arrived(FDA, k)
        arrived(FDB, k)
        return 0

    lax.fori_loop(0, S, landed, 0)

    def drain(kinds, parity=None):
        for kind in kinds:
            for k in range(S - NS, S):
                if parity is None or k % 2 == parity:
                    message(kind, k).wait_send()

    drain((A1, FAY, FDA, FDB))

    @on_inner
    def _():
        drain((A3, FAO))
        drain((B2, B3, FBO, FBI, FB2), 1)
        drain((C2, C3, FC2, FC3), 0)

    @on_outer
    def _():
        drain((A2,))
        drain((B1,), 1)
        drain((C1, C4, FC1), 0)


PIECES = 2


def write_out(*refs):
    sources, targets, sems = refs[:4], refs[4:8], refs[8]
    copies = []
    for i, (source, target) in enumerate(zip(sources, targets)):
        size = source.shape[0] // PIECES
        for j in range(PIECES):
            rows = pl.ds(j * size, size)
            copies.append(pltpu.make_async_copy(source.at[rows, :], target.at[rows, :], sems.at[i, j]))
    for copy in copies:
        copy.start()
    for copy in copies:
        copy.wait()


def solution(mesh):
    def step(x, dy, gate, up, w_gate, w_up, w_down):
        vmem = pltpu.VMEM
        dma = pltpu.SemaphoreType.DMA
        scratch = [
            vmem((M, HALF), F32), vmem((M, HALF), BF16),
            *[vmem((M // 2, WA), BF16)] * 3,
            vmem((M // 2, WB), BF16), *[vmem((M // 2, WB), BF16)] * 2, vmem((M // 4, WB), BF16),
            vmem((2, TB, HALF), BF16),
            *[vmem((NS, H, WA), BF16)] * 3,
            vmem((NS, R, WB), BF16), *[vmem((NS, H, WB), BF16)] * 3,
            vmem((D, 2 * F), BF16), vmem((F, D), BF16),
            vmem((2, TB, D), BF16), vmem((2, TB, F), BF16), vmem((2, TB, F), BF16),
            vmem((M, 2 * F), BF16), vmem((F, M), BF16),
            vmem((2, M, TB), BF16), vmem((TB, M), BF16),
            dma((ROWS, NS)), dma((ROWS, S)), dma((2,)), dma((NB,)), dma((3,)), dma((2, 3)), dma((2,)),
        ]
        anywhere = pl.BlockSpec(memory_space=pl.ANY)
        shape = jax.ShapeDtypeStruct
        shapes = ((M, D), (D, F), (D, F), (F, D))
        grads = pl.pallas_call(
            kernel,
            out_shape=tuple(vmem(dims, BF16) for dims in shapes),
            in_specs=[anywhere] * 7,
            out_specs=(pl.BlockSpec(memory_space=vmem),) * 4,
            scratch_shapes=scratch,
            compiler_params=pltpu.CompilerParams(collective_id=0, has_side_effects=True, vmem_limit_bytes=LIMIT),
        )(x, dy, gate, up, w_gate, w_up, w_down)
        return pl.pallas_call(
            write_out,
            out_shape=tuple(shape(dims, BF16) for dims in shapes),
            in_specs=[pl.BlockSpec(memory_space=vmem)] * 4,
            out_specs=(anywhere,) * 4,
            scratch_shapes=[dma((4, PIECES))],
            compiler_params=pltpu.CompilerParams(vmem_limit_bytes=1 << 20),
        )(*grads)

    tokens, columns, rows = P("dp", None), P(None, "tp"), P("tp", None)
    return jax.shard_map(
        step,
        mesh=mesh,
        in_specs=(tokens, tokens, P("dp", "tp"), P("dp", "tp"), columns, columns, rows),
        out_specs=(tokens, P("dp", "tp"), P("dp", "tp"), P(("dp", "tp"), None)),
        check_vma=False,
    )
```
